128 devices in a mesh: gx: 4 (over x), gy: 4 (over z), gz: 8 (over y, core).
Axes of the slice: x: 4, y: 4, z: 4, core: 2. Of those that a mesh axis runs over, the one named last changes fastest.
Arguments:
- right_side: float32 [3, 32, 128, 1024], P(None, 'gx', 'gy', 'gz'), may hold values from -6 to 6
- mass_coef: float32 [3, 32, 128, 1024], P(None, 'gx', 'gy', 'gz'), may hold values from 0.3 to 3
- curl_coef: float32 [3, 32, 128, 1024], P(None, 'gx', 'gy', 'gz'), may hold values from 0.5 to 5
Outputs:
- solution: float32 [3, 32, 128, 1024], P(None, 'gx', 'gy', 'gz')
- residual: float32 [3, 32, 128, 1024], P(None, 'gx', 'gy', 'gz')
The draws below stay inside these ranges and needn't reach their ends.
All inputs are finite; a program needn't handle non-finite values.
Results may differ from the reference program's by a relative error of at most 0.0003.
Values sent between devices are 32-bit elements; how exact they have to be, the bound alone decides.
A program may use at most 64 MiB of HBM per device.

```python
import math
import jax
import jax.numpy as jnp
from jax import lax

ITERS = 4
NX = 32
NY = 128
NZ = 1024


def block_levels(own_key, dims, split, smallest, largest):
    gain = 1.0
    for axis_at, parts in split:
        draws = jax.random.uniform(jax.random.fold_in(jax.random.fold_in(own_key, 6), axis_at), (parts,), jnp.float32, smallest / len(split), largest / len(split))
        gain = gain * jnp.repeat(jnp.exp(draws), dims[axis_at] // parts).reshape((-1,) + (1,) * (len(dims) - 1 - axis_at))
    return gain


def bell_draw(own_key, extent, spread, limit, split=(), held_as=jnp.bfloat16):
    loudness = block_levels(own_key, extent, split, -0.22, 0.18) if split else 1.0
    result = jax.random.normal(own_key, extent, jnp.float32) * spread * loudness
    return jnp.minimum(jnp.maximum(result, -limit), limit).astype(held_as)


def setup_inputs(seed: int = 0) -> dict:
    keys = jax.random.split(jax.random.key(seed), 4)
    return {
        "right_side": bell_draw(keys[0], (3, NX, NY, NZ), 1.0, 6.0, ((1, 4), (2, 4), (3, 8)), jnp.float32),
        "mass_coef": jnp.clip(jnp.exp(math.log(3.0) - 2.3025851 * jax.random.uniform(keys[1], (3, NX, NY, NZ), jnp.float32) ** block_levels(keys[1], (3, NX, NY, NZ), ((1, 4), (2, 4), (3, 8)), -0.2, 0.2)), 0.3, 3.0),
        "curl_coef": jnp.clip(jnp.exp(math.log(5.0) - 2.3025851 * jax.random.uniform(keys[2], (3, NX, NY, NZ), jnp.float32) ** block_levels(keys[2], (3, NX, NY, NZ), ((1, 4), (2, 4), (3, 8)), -0.2, 0.2)), 0.5, 5.0),
    }


def region(values, start, size):
    return lax.slice(values, tuple(start), tuple(s + n for s, n in zip(start, size)))


def shifted(values, size, base, dim, delta):
    start = [base, base, base]
    if dim >= 0:
        start[dim] = start[dim] + delta
    return region(values, start, size)


def apply_curl(padded, sigma_pad, mu_pad):
    inner = tuple(n - 2 for n in padded.shape[1:])
    faces = tuple(n - 1 for n in padded.shape[1:])
    along_x, along_y, along_z = padded[0], padded[1], padded[2]

    def face_at(values, dim):
        return shifted(values, faces, 0, dim, 1)

    def out_at(values, dim):
        return shifted(values, inner, 1, dim, -1)

    flux_x = (face_at(along_z, 1) - face_at(along_z, -1)) - (face_at(along_y, 2) - face_at(along_y, -1))
    flux_y = (face_at(along_x, 2) - face_at(along_x, -1)) - (face_at(along_z, 0) - face_at(along_z, -1))
    flux_z = (face_at(along_y, 0) - face_at(along_y, -1)) - (face_at(along_x, 1) - face_at(along_x, -1))
    weighted_x = face_at(mu_pad[0], -1) * flux_x
    weighted_y = face_at(mu_pad[1], -1) * flux_y
    weighted_z = face_at(mu_pad[2], -1) * flux_z
    result_x = (out_at(weighted_y, 2) - out_at(weighted_y, -1)) - (out_at(weighted_z, 1) - out_at(weighted_z, -1)) + out_at(sigma_pad[0], -1) * out_at(along_x, -1)
    result_y = (out_at(weighted_z, 0) - out_at(weighted_z, -1)) - (out_at(weighted_x, 2) - out_at(weighted_x, -1)) + out_at(sigma_pad[1], -1) * out_at(along_y, -1)
    result_z = (out_at(weighted_x, 1) - out_at(weighted_x, -1)) - (out_at(weighted_y, 0) - out_at(weighted_y, -1)) + out_at(sigma_pad[2], -1) * out_at(along_z, -1)
    return jnp.stack([result_x, result_y, result_z])


def edge_inverse(sigma_pad, mu_pad):
    inner = tuple(n - 2 for n in sigma_pad.shape[1:])

    def out_at(values, dim):
        return shifted(values, inner, 1, dim, -1)

    diag_x = out_at(sigma_pad[0], -1) + out_at(mu_pad[1], -1) + out_at(mu_pad[1], 2) + out_at(mu_pad[2], -1) + out_at(mu_pad[2], 1)
    diag_y = out_at(sigma_pad[1], -1) + out_at(mu_pad[2], -1) + out_at(mu_pad[2], 0) + out_at(mu_pad[0], -1) + out_at(mu_pad[0], 2)
    diag_z = out_at(sigma_pad[2], -1) + out_at(mu_pad[0], -1) + out_at(mu_pad[0], 1) + out_at(mu_pad[1], -1) + out_at(mu_pad[1], 0)
    return 1.0 / jnp.stack([diag_x, diag_y, diag_z])


def node_inverse(sigma_pad):
    nodes = tuple(n - 1 for n in sigma_pad.shape[1:])
    total = jnp.zeros(nodes, jnp.float32)
    for comp in range(3):
        total = total + shifted(sigma_pad[comp], nodes, 1, -1, 0) + shifted(sigma_pad[comp], nodes, 1, comp, -1)
    return 1.0 / total


def apply_aux(padded, edge_inv, node_inv):
    nodes = tuple(n - 1 for n in padded.shape[1:])
    inner = tuple(n - 2 for n in padded.shape[1:])
    nodal = jnp.zeros(nodes, jnp.float32)
    for comp in range(3):
        nodal = nodal + shifted(padded[comp], nodes, 1, comp, -1) - shifted(padded[comp], nodes, 1, -1, 0)
    potential = nodal * node_inv
    gradient = jnp.stack([shifted(potential, inner, 0, comp, 1) - shifted(potential, inner, 0, -1, 0) for comp in range(3)])
    return padded[:, 1:-1, 1:-1, 1:-1] * edge_inv + gradient


def wrap_pad(values):
    return jnp.pad(values, ((0, 0), (1, 1), (1, 1), (1, 1)), mode="wrap")


def reference(right_side, mass_coef, curl_coef):
    sigma_pad = wrap_pad(mass_coef)
    mu_pad = wrap_pad(curl_coef)
    edge_inv = edge_inverse(sigma_pad, mu_pad)
    node_inv = node_inverse(sigma_pad)

    def pair(values):
        precond = apply_aux(wrap_pad(values), edge_inv, node_inv)
        return precond, apply_curl(wrap_pad(precond), sigma_pad, mu_pad)

    solution = jnp.zeros_like(right_side)
    residual = right_side
    precond_res, image_res = pair(residual)
    direction = jnp.zeros_like(right_side)
    dir_image = jnp.zeros_like(right_side)
    dir_precond = jnp.zeros_like(right_side)
    dir_double = jnp.zeros_like(right_side)
    gamma_old = jnp.float32(1.0)
    alpha_old = jnp.float32(1.0)
    for iteration in range(ITERS):
        gamma_now = jnp.sum(residual * precond_res)
        delta_now = jnp.sum(image_res * precond_res)
        precond_img, image_img = pair(image_res)
        if iteration == 0:
            beta_now = jnp.float32(0.0)
            alpha_now = gamma_now / delta_now
        else:
            beta_now = gamma_now / gamma_old
            alpha_now = gamma_now / (delta_now - beta_now * gamma_now / alpha_old)
        dir_double = image_img + beta_now * dir_double
        dir_precond = precond_img + beta_now * dir_precond
        dir_image = image_res + beta_now * dir_image
        direction = precond_res + beta_now * direction
        solution = solution + alpha_now * direction
        residual = residual - alpha_now * dir_image
        precond_res = precond_res - alpha_now * dir_precond
        image_res = image_res - alpha_now * dir_double
        gamma_old = gamma_now
        alpha_old = alpha_now
    return solution, residual
```

```python
import functools
import jax
import jax.numpy as jnp
from jax import lax
from jax.experimental import pallas as pl
from jax.experimental.pallas import tpu as pltpu
from jax.sharding import PartitionSpec as P

ITERS = 4
THETA = 1.25
SIGMA = 1.25
MESH = pl.DeviceIdType.MESH
F32 = jnp.float32
NB = 8
ROWS = 32
LANES = 128
BASE = 8

ROUND = (
    (1, 0, 0),
    (-1, 0, 0),
    (0, 1, 0),
    (0, -1, 0),
    (0, 0, 1),
    (0, 0, -1),
    (1, -1, 0),
    (-1, 1, 0),
    (1, 0, -1),
    (-1, 0, 1),
    (0, 1, -1),
    (0, -1, 1),
)


def lane_id(rows=ROWS):
    return lax.broadcasted_iota(jnp.int32, (rows, LANES), 1)


def row_id(rows=ROWS):
    return lax.broadcasted_iota(jnp.int32, (rows, LANES), 0)


def roll(v, amount, axis):
    amount = amount % v.shape[axis]
    return v if amount == 0 else pltpu.roll(v, amount, axis)


def place(field, plane):
    return 16 * field + 2 * plane


def packed(acc, v, field, plane):
    at = place(field, plane)
    return jnp.where((lane_id() >> 1) == at // 2, roll(v, at - 127, 1), acc)


def below_y(v, row):
    return jnp.where(row_id() == 0, row, roll(v, 1, 0))


def below_z(v, slab, at):
    return jnp.where(lane_id() == 0, roll(slab, -at, 1), roll(v, 1, 1))


def above_z(v, slab, at):
    return jnp.where(lane_id() == 127, roll(slab, 127 - at, 1), roll(v, -1, 1))


def fold(v):
    return v[0:8] + v[8:16] + v[16:24] + v[24:32]


def cheb_coefficients(nu):
    zero = jnp.zeros_like(nu[0])

    def gram(i, j):
        return 0.5 * (nu[i + j] + nu[abs(i - j)])

    def applied(c):
        out = [zero] * (len(c) + 1)
        for i, a in enumerate(c):
            if i == 0:
                out[1] = out[1] + a
            else:
                out[i + 1] = out[i + 1] + 0.5 * a
                out[i - 1] = out[i - 1] + 0.5 * a
        out = [SIGMA * a for a in out]
        for i, a in enumerate(c):
            out[i] = out[i] + THETA * a
        return out

    def dot(c, d):
        total = zero
        for i, a in enumerate(c):
            for j, b in enumerate(d):
                total = total + a * b * gram(i, j)
        return total

    res = [zero + 1.0]
    direction = None
    iterate = [zero] * ITERS
    gamma_old = alpha_old = None
    for iteration in range(ITERS):
        gamma = dot(res, res)
        delta = dot(applied(res), res)
        if iteration == 0:
            alpha = gamma / delta
            direction = list(res)
        else:
            beta = gamma / gamma_old
            alpha = gamma / (delta - beta * gamma / alpha_old)
            direction = [
                a + (beta * direction[i] if i < len(direction) else zero) for i, a in enumerate(res)
            ]
        for i, a in enumerate(direction):
            iterate[i] = iterate[i] + alpha * a
        image = applied(direction)
        res = [(res[i] if i < len(res) else zero) - alpha * a for i, a in enumerate(image)]
        gamma_old, alpha_old = gamma, alpha
    return iterate, res


def kernel(
    sizes,
    r_hbm,
    m_hbm,
    k_hbm,
    x_out,
    res_out,
    V,
    M,
    K,
    ID,
    IDN,
    F,
    U,
    CX,
    CYS,
    CY,
    CZS,
    CZ,
    YS,
    YR,
    ZS,
    ZR,
    YZR,
    MOM,
    RA,
    SB,
    RB,
    XO,
    RO,
    load_sem,
    c_send,
    c_recv,
    n_send,
    n_recv,
    a_send,
    a_recv,
):
    nx, ny, nz = sizes
    gx, gy, gz = lax.axis_index("gx"), lax.axis_index("gy"), lax.axis_index("gz")

    def device(dx, dy, dz):
        return {
            "gx": lax.rem(gx + dx + nx, nx),
            "gy": lax.rem(gy + dy + ny, ny),
            "gz": lax.rem(gz + dz + nz, nz),
        }

    def remote(src, dst, send, recv, offset):
        return pltpu.make_async_remote_copy(
            src_ref=src,
            dst_ref=dst,
            send_sem=send,
            recv_sem=recv,
            device_id=device(*offset),
            device_id_type=MESH,
        )

    loads = [
        pltpu.make_async_copy(k_hbm, K, load_sem.at[0]),
        pltpu.make_async_copy(m_hbm, M, load_sem.at[1]),
        pltpu.make_async_copy(r_hbm, V.at[0], load_sem.at[2]),
    ]
    for c in loads:
        c.start()
    barrier = pltpu.get_barrier_semaphore()
    for o in ROUND:
        pl.semaphore_signal(barrier, inc=1, device_id=device(*o), device_id_type=MESH)
    for c in loads:
        c.wait()
    y_fields = (K.at[0], K.at[2], M.at[1], V.at[0, 1])
    z_fields = (K.at[0], K.at[1], M.at[2], V.at[0, 2])
    for f, ref in enumerate(y_fields):
        for i in range(NB):
            CYS[f, i : i + 1, :] = ref[i, 31:32, :]
    slab = jnp.zeros((ROWS, LANES), F32)
    for f, ref in enumerate(z_fields):
        for i in range(NB):
            slab = packed(slab, ref[i], f, i)
    CZS[...] = slab
    pl.semaphore_wait(barrier, len(ROUND))
    coef = [
        remote(K.at[1:3, NB - 1], CX.at[0:2], c_send.at[0], c_recv.at[0], (1, 0, 0)),
        remote(M.at[0, NB - 1], CX.at[2], c_send.at[1], c_recv.at[1], (1, 0, 0)),
        remote(V.at[0, 0, NB - 1], CX.at[3], c_send.at[2], c_recv.at[2], (1, 0, 0)),
        remote(CYS, CY, c_send.at[3], c_recv.at[3], (0, 1, 0)),
        remote(CZS, CZ, c_send.at[4], c_recv.at[4], (0, 0, 1)),
    ]
    for c in coef:
        c.start()
    for c in coef:
        c.wait()

    def finish(j, i, slab, values):
        for f, v in enumerate(values):
            F[j, f, 1 + i, BASE : BASE + ROWS, :] = v
            YS[j, f, i : i + 1, :] = v[31:32]
            if f != 1:
                YS[j, (4, 0, 5, 6)[f], i : i + 1, :] = v[0:1]
            slab = packed(slab, v, f, i)
        return slab

    slab = jnp.zeros((ROWS, LANES), F32)
    cz = CZ[...]
    k1_lo, k2_lo, m0_lo, r0_lo = CX[0], CX[1], CX[2], CX[3]
    for i in range(NB):
        k0, k1, k2 = K[0, i], K[1, i], K[2, i]
        m0, m1, m2 = M[0, i], M[1, i], M[2, i]
        r0, r1, r2 = V[0, 0, i], V[0, 1, i], V[0, 2, i]
        k0y = below_y(k0, CY[0, i : i + 1, :])
        k2y = below_y(k2, CY[1, i : i + 1, :])
        m1y = below_y(m1, CY[2, i : i + 1, :])
        r1y = below_y(r1, CY[3, i : i + 1, :])
        k0z = below_z(k0, cz, place(0, i))
        k1z = below_z(k1, cz, place(1, i))
        m2z = below_z(m2, cz, place(2, i))
        r2z = below_z(r2, cz, place(3, i))
        id0 = 1.0 / (m0 + k1 + k1z + k2 + k2y)
        id1 = 1.0 / (m1 + k2 + k2_lo + k0 + k0z)
        id2 = 1.0 / (m2 + k0 + k0y + k1 + k1_lo)
        idn = 1.0 / (m0 + m0_lo + m1 + m1y + m2 + m2z)
        phi = idn * ((r0_lo - r0) + (r1y - r1) + (r2z - r2))
        ID[0, i], ID[1, i], ID[2, i], IDN[i] = id0, id1, id2, idn
        slab = finish(0, i, slab, (r0 * id0, r1 * id1, r2 * id2, phi))
        k1_lo, k2_lo, m0_lo, r0_lo = k1, k2, m0, r0
    ZS[0] = slab

    def messages(j):
        pairs = (
            (F.at[j, 0:4, NB, BASE : BASE + ROWS], F.at[j, 0:4, 0, BASE : BASE + ROWS]),
            (F.at[j, 1:4, 1, BASE : BASE + ROWS], F.at[j, 1:4, NB + 1, BASE : BASE + ROWS]),
            (YS.at[j, 0:4], YR.at[j, 0:4]),
            (YS.at[j, 4:7], YR.at[j, 4:7]),
            (ZS.at[j], ZR.at[j, 0]),
            (ZS.at[j], ZR.at[j, 1]),
            (YS.at[j, 4], YR.at[j, 7]),
            (YS.at[j, 1], YR.at[j, 8]),
            (ZS.at[j], ZR.at[j, 2]),
            (ZS.at[j], ZR.at[j, 3]),
            (ZS.at[j, 24:32], YZR.at[j, 0]),
            (ZS.at[j, 0:8], YZR.at[j, 1]),
        )
        return [
            remote(src, dst, n_send.at[j, k], n_recv.at[j, k], ROUND[k])
            for k, (src, dst) in enumerate(pairs)
        ]

    def one_round(j, carry):
        copies = messages(j)
        for c in copies:
            c.start()
        for c in copies:
            c.wait()
        first = j == 0
        scale = jnp.where(first, F32(1.0 / SIGMA), F32(2.0 / SIGMA))
        back = jnp.where(first, F32(0.0), F32(1.0))
        before = jnp.maximum(j - 1, 0)
        for f, at in ((0, 4), (2, 5), (3, 6)):
            for i in range(NB):
                F[j, f, 1 + i, BASE + ROWS : BASE + ROWS + 1, :] = YR[j, at, i : i + 1, :]
        F[j, 0, 0, BASE + ROWS : BASE + ROWS + 1, :] = YR[j, 7, 7:8, :]
        sub, lane8 = row_id(8), lane_id(8)
        s0, s1, s2, ph = YR[j, 0], YR[j, 1], YR[j, 2], YR[j, 3]
        own0, own2, own_ph = YS[j, 4], YS[j, 5], YS[j, 6]
        s1x = jnp.where(sub == 7, YR[j, 8, 0:1, :], roll(s1, -1, 0))
        corner = jnp.where(lane8 == place(1, sub) + 1, YZR[j, 0, 7:8, :], 0.0)
        corner = jnp.sum(corner, axis=1, keepdims=True)
        s1z = jnp.where(lane8 == 127, corner, roll(s1, -1, 1))
        CYS[0] = CY[0] * ((own2 - s2) - (s1z - s1))
        CYS[1] = CY[1] * ((s1x - s1) - (own0 - s0))
        CYS[2] = CY[2] * (s1 + (own_ph - ph))
        lane, row = lane_id(), row_id()
        low = jnp.where((lane & 1) == 1, ZS[j], ZR[j, 0])
        cz = CZ[...]
        z0, z1 = low, roll(low, -16, 1)
        z2, zp = roll(low, -32, 1), roll(low, -48, 1)
        z2y = jnp.where(row == 31, roll(YZR[j, 1, 0:8, :], -32, 1)[0:1], roll(z2, -1, 0))
        z2x = jnp.where(lane == 14, roll(ZR[j, 3], 14 - 32, 1), roll(z2, -2, 1))
        gz0 = cz * ((z2y - z2) - (roll(z1, -1, 1) - z1))
        gz1 = roll(cz, -16, 1) * ((roll(z0, -1, 1) - z0) - (z2x - z2))
        mz2 = roll(cz, -32, 1) * (z2 + (roll(zp, -1, 1) - zp))
        high = ZR[j, 1]

        def field(f, i):
            return F[j, f, 1 + i, BASE : BASE + ROWS, :]

        def above_y(f, i):
            return F[j, f, 1 + i, BASE + 1 : BASE + 1 + ROWS, :]

        e0, e1, e2, ph = field(0, -1), field(1, -1), field(2, -1), field(3, -1)
        n0, n1, n2, nph = field(0, 0), field(1, 0), field(2, 0), field(3, 0)
        e0z = above_z(e0, ZR[j, 2], place(0, 7) + 1)
        g1_lo = CX[0] * ((e0z - e0) - (n2 - e2))
        g2_lo = CX[1] * ((n1 - e1) - (above_y(0, -1) - e0))
        f0_lo = CX[2] * (e0 + (nph - ph))
        slab = jnp.zeros((ROWS, LANES), F32)
        uv = jnp.zeros((8, LANES), F32)
        wu = jnp.zeros((8, LANES), F32)
        for i in range(NB):
            e0, e1, e2, ph = n0, n1, n2, nph
            if i < NB - 1:
                n0 = field(0, i + 1)
            n1, n2, nph = field(1, i + 1), field(2, i + 1), field(3, i + 1)
            e0z = above_z(e0, high, place(0, i) + 1)
            e1z = above_z(e1, high, place(1, i) + 1)
            phz = above_z(ph, high, place(3, i) + 1)
            g0 = K[0, i] * ((above_y(2, i) - e2) - (e1z - e1))
            g1 = K[1, i] * ((e0z - e0) - (n2 - e2))
            g2 = K[2, i] * ((n1 - e1) - (above_y(0, i) - e0))
            d0, d1, d2 = nph - ph, above_y(3, i) - ph, phz - ph
            u0, u1, u2 = e0 + d0, e1 + d1, e2 + d2
            m0, m1, m2 = M[0, i], M[1, i], M[2, i]
            f0, f1, f2 = m0 * u0, m1 * u1, m2 * u2
            g0y = below_y(g0, CYS[0, i : i + 1, :])
            g2y = below_y(g2, CYS[1, i : i + 1, :])
            f1y = below_y(f1, CYS[2, i : i + 1, :])
            g0z = below_z(g0, gz0, 2 * i)
            g1z = below_z(g1, gz1, 2 * i)
            f2z = below_z(f2, mz2, 2 * i)
            w0 = (g1z - g1) - (g2y - g2) + f0
            w1 = (g2_lo - g2) - (g0z - g0) + f1
            w2 = (g0y - g0) - (g1_lo - g1) + f2
            q = IDN[i] * ((f0_lo - f0) + (f1y - f1) + (f2z - f2))
            v0, v1, v2 = V[j, 0, i], V[j, 1, i], V[j, 2, i]
            U[j, 0, i], U[j, 1, i], U[j, 2, i] = u0, u1, u2
            w0 = scale * (w0 - THETA * v0) - back * V[before, 0, i]
            w1 = scale * (w1 - THETA * v1) - back * V[before, 1, i]
            w2 = scale * (w2 - THETA * v2) - back * V[before, 2, i]
            q = scale * (q - THETA * ph) - back * F[before, 3, 1 + i, BASE : BASE + ROWS, :]
            V[j + 1, 0, i], V[j + 1, 1, i], V[j + 1, 2, i] = w0, w1, w2
            uv = uv + fold(v0 * u0 + v1 * u1 + v2 * u2)
            wu = wu + fold(w0 * u0 + w1 * u1 + w2 * u2)
            slab = finish(j + 1, i, slab, (w0 * ID[0, i], w1 * ID[1, i], w2 * ID[2, i], q))
            g1_lo, g2_lo, f0_lo = g1, g2, f0
        ZS[j + 1] = slab
        MOM[pl.ds(2 * j, 1), :] = jnp.sum(uv, axis=0, keepdims=True)
        MOM[pl.ds(2 * j + 1, 1), :] = jnp.sum(wu, axis=0, keepdims=True)
        return carry

    lax.fori_loop(0, ITERS, one_round, 0)

    core = lax.rem(gz, 2)
    group_a = [(dx, dc) for dx in range(nx) for dc in range(2) if (dx, dc) != (0, 0)]
    copies = []
    for k, (dx, dc) in enumerate(group_a):
        dz = 0 if dc == 0 else 1 - 2 * core
        copies.append(remote(MOM, RA.at[k], a_send.at[k], a_recv.at[k], (dx, 0, dz)))
    for c in copies:
        c.start()
    for c in copies:
        c.wait()
    total = MOM[...]
    for k in range(len(group_a)):
        total = total + RA[k]
    SB[...] = total
    group_b = [(dy, dz) for dy in range(ny) for dz in range(0, nz, 2) if (dy, dz) != (0, 0)]
    copies = []
    for k, (dy, dz) in enumerate(group_b):
        s = len(group_a) + k
        copies.append(remote(SB, RB.at[k], a_send.at[s], a_recv.at[s], (0, dy, dz)))
    for c in copies:
        c.start()
    for c in copies:
        c.wait()
    total = SB[...]
    for k in range(len(group_b)):
        total = total + RB[k]
    total = jnp.broadcast_to(jnp.sum(total, axis=1, keepdims=True), (8, LANES))
    nu = []
    for j in range(ITERS):
        a, b = total[2 * j : 2 * j + 1], total[2 * j + 1 : 2 * j + 2]
        nu += [a, b] if j == 0 else [2.0 * a - nu[0], 2.0 * b - nu[1]]
    cx, cr = cheb_coefficients(nu)
    for c in range(3):
        for i in range(NB):
            x = cx[0] * U[0, c, i]
            y = cr[0] * V[0, c, i]
            for j in range(1, ITERS):
                x = x + cx[j] * U[j, c, i]
            for j in range(1, ITERS + 1):
                y = y + cr[j] * V[j, c, i]
            XO[c, i] = x
            RO[c, i] = y
    stores = [
        pltpu.make_async_copy(XO, x_out, load_sem.at[3]),
        pltpu.make_async_copy(RO, res_out, load_sem.at[4]),
    ]
    for c in stores:
        c.start()
    for c in stores:
        c.wait()


def body(sizes, right_side, mass_coef, curl_coef):
    shape = right_side.shape
    nx, ny, nz = sizes
    n_a = 2 * nx - 1
    n_b = ny * nz // 2 - 1
    vm = lambda *s: pltpu.VMEM(s, F32)
    dma = lambda *s: pltpu.SemaphoreType.DMA(s)
    return pl.pallas_call(
        functools.partial(kernel, sizes),
        out_shape=(jax.ShapeDtypeStruct(shape, F32),) * 2,
        in_specs=[pl.BlockSpec(memory_space=pl.ANY)] * 3,
        out_specs=[pl.BlockSpec(memory_space=pl.ANY)] * 2,
        scratch_shapes=[
            vm(5, *shape),
            vm(*shape),
            vm(*shape),
            vm(*shape),
            vm(*shape[1:]),
            vm(5, 4, 10, 48, LANES),
            vm(4, *shape),
            vm(4, ROWS, LANES),
            vm(4, 8, LANES),
            vm(4, 8, LANES),
            vm(ROWS, LANES),
            vm(ROWS, LANES),
            vm(5, 7, 8, LANES),
            vm(4, 9, 8, LANES),
            vm(5, ROWS, LANES),
            vm(4, 4, ROWS, LANES),
            vm(4, 2, 8, LANES),
            vm(8, LANES),
            vm(n_a, 8, LANES),
            vm(8, LANES),
            vm(n_b, 8, LANES),
            vm(*shape),
            vm(*shape),
            dma(5),
            dma(5),
            dma(5),
            dma(4, 12),
            dma(4, 12),
            dma(n_a + n_b),
            dma(n_a + n_b),
        ],
        compiler_params=pltpu.CompilerParams(collective_id=0, has_side_effects=True),
    )(right_side, mass_coef, curl_coef)


def solution(mesh):
    sizes = (mesh.shape["gx"], mesh.shape["gy"], mesh.shape["gz"])
    spec = P(None, "gx", "gy", "gz")
    return jax.shard_map(
        functools.partial(body, sizes),
        mesh=mesh,
        in_specs=(spec,) * 3,
        out_specs=(spec,) * 2,
        check_vma=False,
    )
```

```python
import functools
import jax
import jax.numpy as jnp
from jax import lax
from jax.experimental import pallas as pl
from jax.experimental.pallas import tpu as pltpu
from jax.sharding import PartitionSpec as P

ITERS = 4
THETA = 1.25
SIGMA = 1.25
MESH = pl.DeviceIdType.MESH
F32 = jnp.float32
NB = 8
ROWS = 32
LANES = 128
BASE = 8

ROUND = (
    (1, -1, 0),
    (-1, 1, 0),
    (1, 0, -1),
    (-1, 0, 1),
    (1, 0, 0),
    (-1, 0, 0),
    (0, 1, -1),
    (0, -1, 1),
    (0, 1, 0),
    (0, -1, 0),
    (0, 0, 1),
    (0, 0, -1),
)
EARLY = range(0, 6)
LATE = range(6, 12)
FACES = ((1, 0, 0), (-1, 0, 0), (0, 1, 0), (0, -1, 0), (0, 0, 1), (0, 0, -1))
ORDER = (7, 0, 1, 2, 3, 4, 5, 6)


def lane_id(rows=ROWS):
    return lax.broadcasted_iota(jnp.int32, (rows, LANES), 1)


def row_id(rows=ROWS):
    return lax.broadcasted_iota(jnp.int32, (rows, LANES), 0)


def roll(v, amount, axis):
    amount = amount % v.shape[axis]
    return v if amount == 0 else pltpu.roll(v, amount, axis)


def place(field, plane):
    return 16 * field + 2 * plane


def packed(acc, v, field, plane):
    at = place(field, plane)
    return jnp.where((lane_id() >> 1) == at // 2, roll(v, at - 127, 1), acc)


def below_y(v, row):
    return jnp.where(row_id() == 0, row, roll(v, 1, 0))


def below_z(v, slab, at):
    return jnp.where(lane_id() == 0, roll(slab, -at, 1), roll(v, 1, 1))


def above_z(v, slab, at):
    return jnp.where(lane_id() == 127, roll(slab, 127 - at, 1), roll(v, -1, 1))


def to_lanes(v, lane):
    out = jnp.zeros((8, LANES), F32)
    for b in range(4):
        out = jnp.where(lane_id(8) == b, roll(v[8 * b : 8 * b + 8], b - lane, 1), out)
    return out


def from_lanes(v, lane):
    return jnp.concatenate([roll(v, lane - b, 1) for b in range(4)], axis=0)


def fold(v):
    return v[0:8] + v[8:16] + v[16:24] + v[24:32]


def cheb_coefficients(nu):
    zero = jnp.zeros_like(nu[0])

    def gram(i, j):
        return 0.5 * (nu[i + j] + nu[abs(i - j)])

    def applied(c):
        out = [zero] * (len(c) + 1)
        for i, a in enumerate(c):
            if i == 0:
                out[1] = out[1] + a
            else:
                out[i + 1] = out[i + 1] + 0.5 * a
                out[i - 1] = out[i - 1] + 0.5 * a
        out = [SIGMA * a for a in out]
        for i, a in enumerate(c):
            out[i] = out[i] + THETA * a
        return out

    def dot(c, d):
        total = zero
        for i, a in enumerate(c):
            for j, b in enumerate(d):
                total = total + a * b * gram(i, j)
        return total

    res = [zero + 1.0]
    direction = None
    iterate = [zero] * ITERS
    gamma_old = alpha_old = None
    for iteration in range(ITERS):
        gamma = dot(res, res)
        delta = dot(applied(res), res)
        if iteration == 0:
            alpha = gamma / delta
            direction = list(res)
        else:
            beta = gamma / gamma_old
            alpha = gamma / (delta - beta * gamma / alpha_old)
            direction = [
                a + (beta * direction[i] if i < len(direction) else zero) for i, a in enumerate(res)
            ]
        for i, a in enumerate(direction):
            iterate[i] = iterate[i] + alpha * a
        image = applied(direction)
        res = [(res[i] if i < len(res) else zero) - alpha * a for i, a in enumerate(image)]
        gamma_old, alpha_old = gamma, alpha
    return iterate, res


def kernel(
    sizes,
    r_hbm,
    m_hbm,
    k_hbm,
    x_out,
    res_out,
    V,
    M,
    K,
    ID,
    IDN,
    F,
    U,
    G,
    CX,
    CYS,
    CY,
    CZS,
    CZ,
    YS,
    YR,
    ZS,
    ZR,
    DS,
    DR,
    LOW,
    MOM,
    RA,
    SB,
    RB,
    load_sem,
    c_send,
    c_recv,
    n_send,
    n_recv,
    a_send,
    a_recv,
):
    nx, ny, nz = sizes
    gx, gy, gz = lax.axis_index("gx"), lax.axis_index("gy"), lax.axis_index("gz")

    def device(dx, dy, dz):
        return {
            "gx": lax.rem(gx + dx + nx, nx),
            "gy": lax.rem(gy + dy + ny, ny),
            "gz": lax.rem(gz + dz + nz, nz),
        }

    def remote(src, dst, send, recv, offset):
        return pltpu.make_async_remote_copy(
            src_ref=src,
            dst_ref=dst,
            send_sem=send,
            recv_sem=recv,
            device_id=device(*offset),
            device_id_type=MESH,
        )

    loads = [
        pltpu.make_async_copy(k_hbm, K, load_sem.at[0]),
        pltpu.make_async_copy(m_hbm, M, load_sem.at[1]),
        pltpu.make_async_copy(r_hbm, V.at[0], load_sem.at[2]),
    ]
    for c in loads:
        c.start()
    barrier = pltpu.get_barrier_semaphore()
    for o in FACES:
        pl.semaphore_signal(barrier, inc=1, device_id=device(*o), device_id_type=MESH)
    for c in loads:
        c.wait()
    y_fields = (K.at[0], K.at[2], M.at[1], V.at[0, 1])
    z_fields = (K.at[0], K.at[1], M.at[2], V.at[0, 2])
    for f, ref in enumerate(y_fields):
        for i in range(NB):
            CYS[f, i : i + 1, :] = ref[i, 31:32, :]
    slab = jnp.zeros((ROWS, LANES), F32)
    for f, ref in enumerate(z_fields):
        for i in range(NB):
            slab = packed(slab, ref[i], f, i)
    CZS[...] = slab
    pl.semaphore_wait(barrier, len(FACES))
    coef = [
        remote(K.at[1:3, NB - 1], CX.at[0:2], c_send.at[0], c_recv.at[0], (1, 0, 0)),
        remote(M.at[0, NB - 1], CX.at[2], c_send.at[1], c_recv.at[1], (1, 0, 0)),
        remote(V.at[0, 0, NB - 1], CX.at[3], c_send.at[2], c_recv.at[2], (1, 0, 0)),
        remote(CYS, CY, c_send.at[3], c_recv.at[3], (0, 1, 0)),
        remote(CZS, CZ, c_send.at[4], c_recv.at[4], (0, 0, 1)),
    ]
    for c in coef:
        c.start()
    for c in coef:
        c.wait_recv()

    def messages(j, which):
        pairs = (
            (DS.at[j, 0], DR.at[j, 0]),
            (DS.at[j, 1], DR.at[j, 1]),
            (DS.at[j, 2], DR.at[j, 2]),
            (DS.at[j, 3], DR.at[j, 3]),
            (F.at[j, 0:4, NB, BASE : BASE + ROWS], F.at[j, 0:4, 0, BASE : BASE + ROWS]),
            (F.at[j, 1:4, 1, BASE : BASE + ROWS], F.at[j, 1:4, NB + 1, BASE : BASE + ROWS]),
            (YS.at[j, 1], DR.at[j, 4]),
            (ZS.at[j, 0:8], DR.at[j, 5]),
            (YS.at[j, 0:4], YR.at[j, 0:4]),
            (YS.at[j, 4:7], YR.at[j, 4:7]),
            (ZS.at[j], ZR.at[j, 0]),
            (ZS.at[j], ZR.at[j, 1]),
        )
        return [
            remote(*pairs[k], n_send.at[j, k], n_recv.at[j, k], ROUND[k]) for k in which
        ]

    def send(j, which):
        for c in messages(j, which):
            c.start()

    def receive(j):
        for c in messages(j, (0, 1, 2, 3, 6, 7, 8, 9, 10, 11, 4, 5)):
            c.wait_recv()

    def finish(j, i, slab, values):
        for f, v in enumerate(values):
            F[j, f, 1 + i, BASE : BASE + ROWS, :] = v
            YS[j, f, i : i + 1, :] = v[31:32]
            if f != 1:
                YS[j, (4, 0, 5, 6)[f], i : i + 1, :] = v[0:1]
            slab = packed(slab, v, f, i)
        if i == NB - 1:
            DS[j, 0] = jnp.broadcast_to(values[0][0:1], (8, LANES))
            DS[j, 2] = to_lanes(values[0], 0)
        if i == 0:
            DS[j, 1] = jnp.broadcast_to(values[1][31:32], (8, LANES))
            DS[j, 3] = to_lanes(values[2], 127)
        return slab

    slab = jnp.zeros((ROWS, LANES), F32)
    cz = CZ[...]
    for i in ORDER:
        k0, k1, k2 = K[0, i], K[1, i], K[2, i]
        m0, m1, m2 = M[0, i], M[1, i], M[2, i]
        r0, r1, r2 = V[0, 0, i], V[0, 1, i], V[0, 2, i]
        if i == 0:
            k1_lo, k2_lo, m0_lo, r0_lo = CX[0], CX[1], CX[2], CX[3]
        else:
            k1_lo, k2_lo, m0_lo, r0_lo = K[1, i - 1], K[2, i - 1], M[0, i - 1], V[0, 0, i - 1]
        k0y = below_y(k0, CY[0, i : i + 1, :])
        k2y = below_y(k2, CY[1, i : i + 1, :])
        m1y = below_y(m1, CY[2, i : i + 1, :])
        r1y = below_y(r1, CY[3, i : i + 1, :])
        k0z = below_z(k0, cz, place(0, i))
        k1z = below_z(k1, cz, place(1, i))
        m2z = below_z(m2, cz, place(2, i))
        r2z = below_z(r2, cz, place(3, i))
        id0 = 1.0 / (m0 + k1 + k1z + k2 + k2y)
        id1 = 1.0 / (m1 + k2 + k2_lo + k0 + k0z)
        id2 = 1.0 / (m2 + k0 + k0y + k1 + k1_lo)
        idn = 1.0 / (m0 + m0_lo + m1 + m1y + m2 + m2z)
        phi = idn * ((r0_lo - r0) + (r1y - r1) + (r2z - r2))
        ID[0, i], ID[1, i], ID[2, i], IDN[i] = id0, id1, id2, idn
        slab = finish(0, i, slab, (r0 * id0, r1 * id1, r2 * id2, phi))
        if i == 0:
            send(0, EARLY)
    ZS[0] = slab
    send(0, LATE)

    def field(j, f, i):
        return F[j, f, 1 + i, BASE : BASE + ROWS, :]

    def above_y(j, f, i):
        return F[j, f, 1 + i, BASE + 1 : BASE + 1 + ROWS, :]

    def edges(j):
        for f, at in ((0, 4), (2, 5), (3, 6)):
            for i in range(NB):
                F[j, f, 1 + i, BASE + ROWS : BASE + ROWS + 1, :] = YR[j, at, i : i + 1, :]
        F[j, 0, 0, BASE + ROWS : BASE + ROWS + 1, :] = DR[j, 0, 0:1, :]
        sub, lane8 = row_id(8), lane_id(8)
        s0, s1, s2, ph = YR[j, 0], YR[j, 1], YR[j, 2], YR[j, 3]
        own0, own2, own_ph = YS[j, 4], YS[j, 5], YS[j, 6]
        s1x = jnp.where(sub == 7, DR[j, 1], roll(s1, -1, 0))
        s1z = jnp.where(lane8 == 127, roll(DR[j, 4], -1, 1), roll(s1, -1, 1))
        LOW[0] = CY[0] * ((own2 - s2) - (s1z - s1))
        LOW[1] = CY[1] * ((s1x - s1) - (own0 - s0))
        LOW[2] = CY[2] * (s1 + (own_ph - ph))
        lane, row = lane_id(), row_id()
        low = jnp.where((lane & 1) == 1, ZS[j], ZR[j, 0])
        z0, z1 = low, roll(low, -16, 1)
        z2, zp = roll(low, -32, 1), roll(low, -48, 1)
        z2y = jnp.where(row == 31, roll(DR[j, 5], -32, 1)[0:1], roll(z2, -1, 0))
        z2x = jnp.where(lane == 14, from_lanes(DR[j, 3], 14), roll(z2, -2, 1))
        gz0 = cz * ((z2y - z2) - (roll(z1, -1, 1) - z1))
        gz1 = roll(cz, -16, 1) * ((roll(z0, -1, 1) - z0) - (z2x - z2))
        mz2 = roll(cz, -32, 1) * (z2 + (roll(zp, -1, 1) - zp))
        return gz0, gz1, mz2, ZR[j, 1]

    def fluxes_low(j):
        e0, e1, e2, ph = (field(j, f, -1) for f in range(4))
        n1, n2, nph = (field(j, f, 0) for f in (1, 2, 3))
        e0z = jnp.where(lane_id() == 127, from_lanes(DR[j, 2], 127), roll(e0, -1, 1))
        g1 = CX[0] * ((e0z - e0) - (n2 - e2))
        g2 = CX[1] * ((n1 - e1) - (above_y(j, 0, -1) - e0))
        return g1, g2, CX[2] * (e0 + (nph - ph))

    def fluxes_before(j, i, high):
        e0, e1, e2, ph = (field(j, f, i) for f in range(4))
        n1, n2, nph = (field(j, f, i + 1) for f in (1, 2, 3))
        e0z = above_z(e0, high, place(0, i) + 1)
        g1 = K[1, i] * ((e0z - e0) - (n2 - e2))
        g2 = K[2, i] * ((n1 - e1) - (above_y(j, 0, i) - e0))
        return g1, g2, M[0, i] * (e0 + (nph - ph))

    def fluxes(j, i, high):
        e0, e1, e2, ph = (field(j, f, i) for f in range(4))
        n1, n2, nph = (field(j, f, i + 1) for f in (1, 2, 3))
        e0z = above_z(e0, high, place(0, i) + 1)
        e1z = above_z(e1, high, place(1, i) + 1)
        phz = above_z(ph, high, place(3, i) + 1)
        c0 = (above_y(j, 2, i) - e2) - (e1z - e1)
        c1 = (e0z - e0) - (n2 - e2)
        c2 = (n1 - e1) - (above_y(j, 0, i) - e0)
        u0 = e0 + (nph - ph)
        u1 = e1 + (above_y(j, 3, i) - ph)
        u2 = e2 + (phz - ph)
        return (c0, c1, c2), (u0, u1, u2)

    def operator(i, g, f, lo, slabs):
        gz0, gz1, mz2, _ = slabs
        g0, g1, g2 = g
        f0, f1, f2 = f
        g1_lo, g2_lo, f0_lo = lo
        g0y = below_y(g0, LOW[0, i : i + 1, :])
        g2y = below_y(g2, LOW[1, i : i + 1, :])
        g0z = below_z(g0, gz0, 2 * i)
        g1z = below_z(g1, gz1, 2 * i)
        w0 = (g1z - g1) - (g2y - g2) + f0
        w1 = (g2_lo - g2) - (g0z - g0) + f1
        w2 = (g0y - g0) - (g1_lo - g1) + f2
        return w0, w1, w2

    def divergence(i, f, lo, slabs):
        f1y = below_y(f[1], LOW[2, i : i + 1, :])
        f2z = below_z(f[2], slabs[2], 2 * i)
        return IDN[i] * ((lo[2] - f[0]) + (f1y - f[1]) + (f2z - f[2]))

    def one_round(j, carry):
        receive(j)
        first = j == 0
        scale = jnp.where(first, F32(1.0 / SIGMA), F32(2.0 / SIGMA))
        back = jnp.where(first, F32(0.0), F32(1.0))
        before = jnp.maximum(j - 1, 0)
        slabs = edges(j)
        high = slabs[3]
        slab = jnp.zeros((ROWS, LANES), F32)
        uv = jnp.zeros((8, LANES), F32)
        wu = jnp.zeros((8, LANES), F32)
        for i in ORDER:
            if i == 7:
                lo = fluxes_before(j, 6, high)
            if i == 0:
                lo = fluxes_low(j)
            c, u = fluxes(j, i, high)
            g = [K[n, i] * c[n] for n in range(3)]
            f = [M[n, i] * u[n] for n in range(3)]
            w = operator(i, g, f, lo, slabs)
            q = divergence(i, f, lo, slabs)
            v = [V[j, n, i] for n in range(3)]
            w = [scale * (w[n] - THETA * v[n]) - back * V[before, n, i] for n in range(3)]
            q = scale * (q - THETA * field(j, 3, i)) - back * field(before, 3, i)
            for n in range(3):
                U[j, n, i] = u[n]
                V[j + 1, n, i] = w[n]
            slab = finish(j + 1, i, slab, [w[n] * ID[n, i] for n in range(3)] + [q])
            uv = uv + fold(v[0] * u[0] + v[1] * u[1] + v[2] * u[2])
            wu = wu + fold(w[0] * u[0] + w[1] * u[1] + w[2] * u[2])
            lo = (g[1], g[2], f[0])
            if i == 0:
                send(j + 1, EARLY)
        ZS[j + 1] = slab
        send(j + 1, LATE)
        MOM[pl.ds(2 * j, 1), :] = jnp.sum(uv, axis=0, keepdims=True)
        MOM[pl.ds(2 * j + 1, 1), :] = jnp.sum(wu, axis=0, keepdims=True)
        return carry

    last = ITERS - 1
    lax.fori_loop(0, last, one_round, 0)

    receive(last)
    slabs = edges(last)
    uv = jnp.zeros((8, LANES), F32)
    au = jnp.zeros((8, LANES), F32)
    bu = jnp.zeros((8, LANES), F32)
    for i in range(NB):
        c, u = fluxes(last, i, slabs[3])
        g = [K[n, i] * c[n] for n in range(3)]
        f = [M[n, i] * u[n] for n in range(3)]
        v = [V[last, n, i] for n in range(3)]
        b = [V[last - 1, n, i] for n in range(3)]
        for n in range(3):
            U[last, n, i] = u[n]
            G[n, i], G[3 + n, i] = g[n], f[n]
        uv = uv + fold(v[0] * u[0] + v[1] * u[1] + v[2] * u[2])
        bu = bu + fold(b[0] * u[0] + b[1] * u[1] + b[2] * u[2])
        au = au + fold(
            (g[0] * c[0] + g[1] * c[1] + g[2] * c[2]) + (f[0] * u[0] + f[1] * u[1] + f[2] * u[2])
        )
    scale = 2.0 / SIGMA
    wu = scale * (au - THETA * uv) - bu
    MOM[2 * last : 2 * last + 1, :] = jnp.sum(uv, axis=0, keepdims=True)
    MOM[2 * last + 1 : 2 * last + 2, :] = jnp.sum(wu, axis=0, keepdims=True)

    def last_planes(planes):
        for i in planes:
            if i == 0:
                lo = fluxes_low(last)
            else:
                lo = (G[1, i - 1], G[2, i - 1], G[3, i - 1])
            w = operator(i, [G[n, i] for n in range(3)], [G[3 + n, i] for n in range(3)], lo, slabs)
            for n in range(3):
                V[last + 1, n, i] = scale * (w[n] - THETA * V[last, n, i]) - V[last - 1, n, i]

    core = lax.rem(gz, 2)
    group_a = [(dx, dc) for dx in range(nx) for dc in range(2) if (dx, dc) != (0, 0)]
    sums_a = []
    for k, (dx, dc) in enumerate(group_a):
        dz = 0 if dc == 0 else 1 - 2 * core
        sums_a.append(remote(MOM, RA.at[k], a_send.at[k], a_recv.at[k], (dx, 0, dz)))
    for c in sums_a:
        c.start()
    last_planes(range(0, 4))
    for c in sums_a:
        c.wait_recv()
    total = MOM[...]
    for k in range(len(group_a)):
        total = total + RA[k]
    SB[...] = total
    group_b = [(dy, dz) for dy in range(ny) for dz in range(0, nz, 2) if (dy, dz) != (0, 0)]
    sums_b = []
    for k, (dy, dz) in enumerate(group_b):
        s = len(group_a) + k
        sums_b.append(remote(SB, RB.at[k], a_send.at[s], a_recv.at[s], (0, dy, dz)))
    for c in sums_b:
        c.start()
    last_planes(range(4, 8))

    def sent(j, carry):
        for c in messages(j, range(12)):
            c.wait_send()
        return carry

    lax.fori_loop(0, ITERS, sent, 0)
    for c in coef + sums_a:
        c.wait_send()
    for c in sums_b:
        c.wait_recv()
    total = SB[...]
    for k in range(len(group_b)):
        total = total + RB[k]
    total = jnp.broadcast_to(jnp.sum(total, axis=1, keepdims=True), (8, LANES))
    nu = []
    for j in range(ITERS):
        a, b = total[2 * j : 2 * j + 1], total[2 * j + 1 : 2 * j + 2]
        nu += [a, b] if j == 0 else [2.0 * a - nu[0], 2.0 * b - nu[1]]
    cx, cr = cheb_coefficients(nu)
    for c in range(3):
        for i in range(NB):
            x = cx[0] * U[0, c, i]
            y = cr[0] * V[0, c, i]
            for j in range(1, ITERS):
                x = x + cx[j] * U[j, c, i]
            for j in range(1, ITERS + 1):
                y = y + cr[j] * V[j, c, i]
            x_out[c, i] = x
            res_out[c, i] = y
    for c in sums_b:
        c.wait_send()


def body(sizes, right_side, mass_coef, curl_coef):
    shape = right_side.shape
    nx, ny, nz = sizes
    n_a = 2 * nx - 1
    n_b = ny * nz // 2 - 1
    vm = lambda *s: pltpu.VMEM(s, F32)
    dma = lambda *s: pltpu.SemaphoreType.DMA(s)
    return pl.pallas_call(
        functools.partial(kernel, sizes),
        out_shape=(pltpu.VMEM(shape, F32),) * 2,
        in_specs=[pl.BlockSpec(memory_space=pl.ANY)] * 3,
        out_specs=[pl.BlockSpec(memory_space=pltpu.VMEM)] * 2,
        scratch_shapes=[
            vm(5, *shape),
            vm(*shape),
            vm(*shape),
            vm(*shape),
            vm(*shape[1:]),
            vm(4, 4, 10, 48, LANES),
            vm(4, *shape),
            vm(6, *shape[1:]),
            vm(4, ROWS, LANES),
            vm(4, 8, LANES),
            vm(4, 8, LANES),
            vm(ROWS, LANES),
            vm(ROWS, LANES),
            vm(4, 7, 8, LANES),
            vm(4, 7, 8, LANES),
            vm(4, ROWS, LANES),
            vm(4, 2, ROWS, LANES),
            vm(4, 4, 8, LANES),
            vm(4, 6, 8, LANES),
            vm(3, 8, LANES),
            vm(8, LANES),
            vm(n_a, 8, LANES),
            vm(8, LANES),
            vm(n_b, 8, LANES),
            dma(3),
            dma(5),
            dma(5),
            dma(4, 12),
            dma(4, 12),
            dma(n_a + n_b),
            dma(n_a + n_b),
        ],
        compiler_params=pltpu.CompilerParams(collective_id=0, has_side_effects=True),
    )(right_side, mass_coef, curl_coef)


def solution(mesh):
    sizes = (mesh.shape["gx"], mesh.shape["gy"], mesh.shape["gz"])
    spec = P(None, "gx", "gy", "gz")
    return jax.shard_map(
        functools.partial(body, sizes),
        mesh=mesh,
        in_specs=(spec,) * 3,
        out_specs=(spec,) * 2,
        check_vma=False,
    )
```

```python
import functools
import jax
import jax.numpy as jnp
from jax import lax
from jax.experimental import pallas as pl
from jax.experimental.pallas import tpu as pltpu
from jax.sharding import PartitionSpec as P

ITERS = 4
THETA = 1.25
SIGMA = 1.25
MESH = pl.DeviceIdType.MESH
F32 = jnp.float32
NB = 8
ROWS = 32
LANES = 128
BASE = 8

ROUND = (
    (1, -1, 0),
    (-1, 1, 0),
    (1, 0, -1),
    (-1, 0, 1),
    (1, 0, 0),
    (-1, 0, 0),
    (0, 1, -1),
    (0, -1, 1),
    (0, 1, 0),
    (0, -1, 0),
    (0, 0, 1),
    (0, 0, -1),
)
EARLY = range(0, 6)
LATE = range(6, 12)
FACES = ((1, 0, 0), (-1, 0, 0), (0, 1, 0), (0, -1, 0), (0, 0, 1), (0, 0, -1))
ORDER = (7, 0, 1, 2, 3, 4, 5, 6)


def lane_id(rows=ROWS):
    return lax.broadcasted_iota(jnp.int32, (rows, LANES), 1)


def row_id(rows=ROWS):
    return lax.broadcasted_iota(jnp.int32, (rows, LANES), 0)


def roll(v, amount, axis):
    amount = amount % v.shape[axis]
    return v if amount == 0 else pltpu.roll(v, amount, axis)


def place(field, plane):
    return 16 * field + 2 * plane


def packed(acc, v, field, plane):
    at = place(field, plane)
    return jnp.where((lane_id() >> 1) == at // 2, roll(v, at - 127, 1), acc)


def below_y(v, row):
    return jnp.where(row_id() == 0, row, roll(v, 1, 0))


def below_z(v, halo):
    return jnp.where(lane_id() == 0, halo, roll(v, 1, 1))


def above_z(v, halo):
    return jnp.where(lane_id() == 127, halo, roll(v, -1, 1))


def lanes_of(parts):
    sums = jnp.sum(parts, axis=1, keepdims=True)
    return jnp.sum(jnp.where(lane_id(8) == row_id(8), sums, 0.0), axis=0, keepdims=True)


def to_lanes(v, lane):
    out = jnp.zeros((8, LANES), F32)
    for b in range(4):
        out = jnp.where(lane_id(8) == b, roll(v[8 * b : 8 * b + 8], b - lane, 1), out)
    return out


def from_lanes(v, lane):
    return jnp.concatenate([roll(v, lane - b, 1) for b in range(4)], axis=0)


def fold(v):
    return v[0:8] + v[8:16] + v[16:24] + v[24:32]


def cheb_coefficients(nu):
    zero = jnp.zeros_like(nu[0])
    top = 2 * ITERS - 1

    def gram(i, j):
        if i + j == top:
            return 0.5 * nu[abs(i - j)]
        return 0.5 * (nu[i + j] + nu[abs(i - j)])

    def applied(c):
        out = [zero] * (len(c) + 1)
        for i, a in enumerate(c):
            if i == 0:
                out[1] = out[1] + a
            else:
                out[i + 1] = out[i + 1] + 0.5 * a
                out[i - 1] = out[i - 1] + 0.5 * a
        out = [SIGMA * a for a in out]
        for i, a in enumerate(c):
            out[i] = out[i] + THETA * a
        return out

    def dot(c, d):
        total = zero
        for i, a in enumerate(c):
            for j, b in enumerate(d):
                total = total + a * b * gram(i, j)
        return total

    res = [zero + 1.0]
    direction = None
    iterate = [zero] * ITERS
    gamma_old = alpha_old = None
    for iteration in range(ITERS):
        gamma = dot(res, res)
        image = applied(res)
        delta = dot(image, res)
        if iteration == 0:
            alpha = gamma / delta
            direction = list(res)
        else:
            beta = gamma / gamma_old
            slack = delta - beta * gamma / alpha_old
            direction = [
                a + (beta * direction[i] if i < len(direction) else zero) for i, a in enumerate(res)
            ]
            if iteration == ITERS - 1:
                return iterate, direction, res, applied(direction), gamma, slack, 0.5 * image[-1] * res[-1]
            alpha = gamma / slack
        for i, a in enumerate(direction):
            iterate[i] = iterate[i] + alpha * a
        step = applied(direction)
        res = [(res[i] if i < len(res) else zero) - alpha * a for i, a in enumerate(step)]
        gamma_old, alpha_old = gamma, alpha


def kernel(
    sizes,
    r_hbm,
    m_hbm,
    k_hbm,
    x_out,
    p_out,
    r_out,
    a_out,
    alpha_out,
    V,
    M,
    K,
    ID,
    IDN,
    F,
    U,
    G,
    XS,
    CX,
    CYS,
    CY,
    CZS,
    CZ,
    CZR,
    YS,
    YR,
    ZS,
    ZR,
    DS,
    DR,
    LOW,
    DN,
    MOM,
    SUM,
    RA,
    RA2,
    RB,
    RB2,
    load_sem,
    c_send,
    c_recv,
    n_send,
    n_recv,
    a_send,
    a_recv,
):
    nx, ny, nz = sizes
    gx, gy, gz = lax.axis_index("gx"), lax.axis_index("gy"), lax.axis_index("gz")

    def device(dx, dy, dz):
        return {
            "gx": lax.rem(gx + dx + nx, nx),
            "gy": lax.rem(gy + dy + ny, ny),
            "gz": lax.rem(gz + dz + nz, nz),
        }

    def remote(src, dst, send, recv, offset):
        return pltpu.make_async_remote_copy(
            src_ref=src,
            dst_ref=dst,
            send_sem=send,
            recv_sem=recv,
            device_id=device(*offset),
            device_id_type=MESH,
        )

    loads = [
        pltpu.make_async_copy(k_hbm, K, load_sem.at[0]),
        pltpu.make_async_copy(m_hbm, M, load_sem.at[1]),
        pltpu.make_async_copy(r_hbm, V.at[0], load_sem.at[2]),
    ]
    first = [
        pltpu.make_async_copy(k_hbm.at[1:3, NB - 1], XS.at[0:2], load_sem.at[3]),
        pltpu.make_async_copy(m_hbm.at[0, NB - 1], XS.at[2], load_sem.at[4]),
        pltpu.make_async_copy(r_hbm.at[0, NB - 1], XS.at[3], load_sem.at[5]),
    ]
    for c in first:
        c.start()
    for c in loads:
        c.start()
    barrier = pltpu.get_barrier_semaphore()
    for o in FACES:
        pl.semaphore_signal(barrier, inc=1, device_id=device(*o), device_id_type=MESH)
    coef = [
        remote(XS, CX, c_send.at[0], c_recv.at[0], (1, 0, 0)),
        remote(CYS, CY, c_send.at[1], c_recv.at[1], (0, 1, 0)),
        remote(CZS, CZ, c_send.at[2], c_recv.at[2], (0, 0, 1)),
    ]
    for c in first:
        c.wait()
    pl.semaphore_wait(barrier, len(FACES))
    coef[0].start()
    for c in loads:
        c.wait()
    y_fields = (K.at[0], K.at[2], M.at[1], V.at[0, 1])
    z_fields = (K.at[0], K.at[1], M.at[2], V.at[0, 2])
    for f, ref in enumerate(y_fields):
        for i in range(NB):
            CYS[f, i : i + 1, :] = ref[i, 31:32, :]
    coef[1].start()
    slab = jnp.zeros((ROWS, LANES), F32)
    for f, ref in enumerate(z_fields):
        for i in range(NB):
            slab = packed(slab, ref[i], f, i)
    CZS[...] = slab
    coef[2].start()
    for c in coef:
        c.wait_recv()

    def messages(j, which):
        pairs = (
            (DS.at[j, 0], DR.at[j, 0]),
            (DS.at[j, 1], DR.at[j, 1]),
            (DS.at[j, 2], DR.at[j, 2]),
            (DS.at[j, 3], DR.at[j, 3]),
            (F.at[j, 0:4, NB, BASE : BASE + ROWS], F.at[j, 0:4, 0, BASE : BASE + ROWS]),
            (F.at[j, 1:4, 1, BASE : BASE + ROWS], F.at[j, 1:4, NB + 1, BASE : BASE + ROWS]),
            (YS.at[j, 1], DR.at[j, 4]),
            (ZS.at[j, 0:8], DR.at[j, 5]),
            (YS.at[j, 0:4], YR.at[j, 0:4]),
            (YS.at[j, 4:7], YR.at[j, 4:7]),
            (ZS.at[j], ZR.at[j, 0]),
            (ZS.at[j], ZR.at[j, 1]),
        )
        return [
            remote(*pairs[k], n_send.at[j, k], n_recv.at[j, k], ROUND[k]) for k in which
        ]

    def send(j, which):
        for c in messages(j, which):
            c.start()

    def receive(j, which):
        for c in messages(j, which):
            c.wait_recv()

    def finish(j, i, slab, values):
        for f, v in enumerate(values):
            F[j, f, 1 + i, BASE : BASE + ROWS, :] = v
            YS[j, f, i : i + 1, :] = v[31:32]
            if f != 1:
                YS[j, (4, 0, 5, 6)[f], i : i + 1, :] = v[0:1]
            slab = packed(slab, v, f, i)
        if i == NB - 1:
            DS[j, 0] = jnp.broadcast_to(values[0][0:1], (8, LANES))
            DS[j, 2] = to_lanes(values[0], 0)
        if i == 0:
            DS[j, 1] = jnp.broadcast_to(values[1][31:32], (8, LANES))
            DS[j, 3] = to_lanes(values[2], 127)
        return slab

    slab = jnp.zeros((ROWS, LANES), F32)
    uv = jnp.zeros((8, LANES), F32)
    cz = CZ[...]
    for f in range(3):
        CZR[f] = roll(cz, 2 - 16 * f, 1)
    for i in ORDER:
        k0, k1, k2 = K[0, i], K[1, i], K[2, i]
        m0, m1, m2 = M[0, i], M[1, i], M[2, i]
        r0, r1, r2 = V[0, 0, i], V[0, 1, i], V[0, 2, i]
        if i == 0:
            k1_lo, k2_lo, m0_lo, r0_lo = CX[0], CX[1], CX[2], CX[3]
        else:
            k1_lo, k2_lo, m0_lo, r0_lo = K[1, i - 1], K[2, i - 1], M[0, i - 1], V[0, 0, i - 1]
        k0y = below_y(k0, CY[0, i : i + 1, :])
        k2y = below_y(k2, CY[1, i : i + 1, :])
        m1y = below_y(m1, CY[2, i : i + 1, :])
        r1y = below_y(r1, CY[3, i : i + 1, :])
        k0z = below_z(k0, roll(cz, -place(0, i), 1))
        k1z = below_z(k1, roll(cz, -place(1, i), 1))
        m2z = below_z(m2, roll(cz, -place(2, i), 1))
        r2z = below_z(r2, roll(cz, -place(3, i), 1))
        id0 = 1.0 / (m0 + k1 + k1z + k2 + k2y)
        id1 = 1.0 / (m1 + k2 + k2_lo + k0 + k0z)
        id2 = 1.0 / (m2 + k0 + k0y + k1 + k1_lo)
        dn = m0 + m0_lo + m1 + m1y + m2 + m2z
        idn = 1.0 / dn
        phi = idn * ((r0_lo - r0) + (r1y - r1) + (r2z - r2))
        ID[0, i], ID[1, i], ID[2, i], IDN[i], DN[i] = id0, id1, id2, idn, dn
        s0, s1, s2 = r0 * id0, r1 * id1, r2 * id2
        slab = finish(0, i, slab, (s0, s1, s2, phi))
        uv = uv + fold(r0 * s0 + r1 * s1 + r2 * s2 + dn * phi * phi)
        if i == 0:
            send(0, EARLY)
    ZS[0] = slab
    send(0, LATE)
    MOM[7:8, :] = jnp.zeros((1, LANES), F32)
    MOM[0:1, :] = jnp.sum(uv, axis=0, keepdims=True)

    def field(j, f, i):
        return F[j, f, 1 + i, BASE : BASE + ROWS, :]

    def above_y(j, f, i):
        return F[j, f, 1 + i, BASE + 1 : BASE + 1 + ROWS, :]

    def rows_above(j):
        for f, at in ((0, 4), (2, 5), (3, 6)):
            for i in range(NB):
                F[j, f, 1 + i, BASE + ROWS : BASE + ROWS + 1, :] = YR[j, at, i : i + 1, :]

    def edges(j):
        F[j, 0, 0, BASE + ROWS : BASE + ROWS + 1, :] = DR[j, 0, 0:1, :]
        sub, lane8 = row_id(8), lane_id(8)
        s0, s1, s2, ph = YR[j, 0], YR[j, 1], YR[j, 2], YR[j, 3]
        own0, own2, own_ph = YS[j, 4], YS[j, 5], YS[j, 6]
        s1x = jnp.where(sub == 7, DR[j, 1], roll(s1, -1, 0))
        s1z = jnp.where(lane8 == 127, roll(DR[j, 4], -1, 1), roll(s1, -1, 1))
        LOW[0] = CY[0] * ((own2 - s2) - (s1z - s1))
        LOW[1] = CY[1] * ((s1x - s1) - (own0 - s0))
        LOW[2] = CY[2] * (s1 + (own_ph - ph))
        lane, row = lane_id(), row_id()
        low = jnp.where((lane & 1) == 1, ZS[j], ZR[j, 0])
        z0, z1, z2, zp = (roll(low, 2 - 16 * f, 1) for f in range(4))
        z2y = jnp.where(row == 31, roll(DR[j, 5], 2 - 32, 1)[0:1], roll(z2, -1, 0))
        z2x = jnp.where(lane == 16, from_lanes(DR[j, 3], 16), roll(z2, -2, 1))
        gz0 = CZR[0] * ((z2y - z2) - (roll(z1, -1, 1) - z1))
        gz1 = CZR[1] * ((roll(z0, -1, 1) - z0) - (z2x - z2))
        mz2 = CZR[2] * (z2 + (roll(zp, -1, 1) - zp))
        odd = (lane & 1) == 1
        high = ZR[j, 1]
        return (
            jnp.where(odd, high, gz1),
            jnp.where(odd, roll(high, -16, 1), gz0),
            jnp.where(odd, roll(high, -48, 1), mz2),
        )

    def halo(slabs, i):
        return [roll(t, 126 - 2 * i, 1) for t in slabs]

    def fluxes_low(j):
        e0, e1, e2, ph = (field(j, f, -1) for f in range(4))
        n1, n2, nph = (field(j, f, 0) for f in (1, 2, 3))
        e0z = jnp.where(lane_id() == 127, from_lanes(DR[j, 2], 127), roll(e0, -1, 1))
        g1 = CX[0] * ((e0z - e0) - (n2 - e2))
        g2 = CX[1] * ((n1 - e1) - (above_y(j, 0, -1) - e0))
        return g1, g2, CX[2] * (e0 + (nph - ph))

    def fluxes_before(j, i, slabs):
        e0, e1, e2, ph = (field(j, f, i) for f in range(4))
        n1, n2, nph = (field(j, f, i + 1) for f in (1, 2, 3))
        e0z = above_z(e0, roll(slabs[0], 126 - 2 * i, 1))
        g1 = K[1, i] * ((e0z - e0) - (n2 - e2))
        g2 = K[2, i] * ((n1 - e1) - (above_y(j, 0, i) - e0))
        return g1, g2, M[0, i] * (e0 + (nph - ph))

    def fluxes(j, i, ends):
        e0, e1, e2, ph = (field(j, f, i) for f in range(4))
        n1, n2, nph = (field(j, f, i + 1) for f in (1, 2, 3))
        e0z = above_z(e0, ends[0])
        e1z = above_z(e1, ends[1])
        phz = above_z(ph, ends[2])
        c0 = (above_y(j, 2, i) - e2) - (e1z - e1)
        c1 = (e0z - e0) - (n2 - e2)
        c2 = (n1 - e1) - (above_y(j, 0, i) - e0)
        u0 = e0 + (nph - ph)
        u1 = e1 + (above_y(j, 3, i) - ph)
        u2 = e2 + (phz - ph)
        return (c0, c1, c2), (u0, u1, u2)

    def operator(i, g, f, lo, ends):
        g0, g1, g2 = g
        f0, f1, f2 = f
        g1_lo, g2_lo, f0_lo = lo
        g0y = below_y(g0, LOW[0, i : i + 1, :])
        g2y = below_y(g2, LOW[1, i : i + 1, :])
        g0z = below_z(g0, ends[1])
        g1z = below_z(g1, ends[0])
        w0 = (g1z - g1) - (g2y - g2) + f0
        w1 = (g2_lo - g2) - (g0z - g0) + f1
        w2 = (g0y - g0) - (g1_lo - g1) + f2
        return w0, w1, w2

    def divergence(i, f, lo, ends):
        f1y = below_y(f[1], LOW[2, i : i + 1, :])
        f2z = below_z(f[2], ends[2])
        return IDN[i] * ((lo[2] - f[0]) + (f1y - f[1]) + (f2z - f[2]))

    def one_round(j, carry):
        receive(j, (0, 1, 2, 3, 6, 7, 8, 9, 10, 11, 4, 5))
        first = j == 0
        scale = jnp.where(first, F32(1.0 / SIGMA), F32(2.0 / SIGMA))
        back = jnp.where(first, F32(0.0), F32(1.0))
        before = jnp.maximum(j - 1, 0)
        rows_above(j)
        slabs = edges(j)
        slab = jnp.zeros((ROWS, LANES), F32)
        uv = jnp.zeros((8, LANES), F32)
        wu = jnp.zeros((8, LANES), F32)
        for i in ORDER:
            if i == 7:
                lo = fluxes_before(j, 6, slabs)
            if i == 0:
                lo = fluxes_low(j)
            ends = halo(slabs, i)
            c, u = fluxes(j, i, ends)
            g = [K[n, i] * c[n] for n in range(3)]
            f = [M[n, i] * u[n] for n in range(3)]
            w = operator(i, g, f, lo, ends)
            q = divergence(i, f, lo, ends)
            v = [V[j, n, i] for n in range(3)]
            w = [scale * (w[n] - THETA * v[n]) - back * V[before, n, i] for n in range(3)]
            q = scale * (q - THETA * field(j, 3, i)) - back * field(before, 3, i)
            for n in range(3):
                U[j, n, i] = u[n]
                V[j + 1, n, i] = w[n]
            s = [w[n] * ID[n, i] for n in range(3)]
            slab = finish(j + 1, i, slab, s + [q])
            uv = uv + fold(w[0] * s[0] + w[1] * s[1] + w[2] * s[2] + DN[i] * q * q)
            wu = wu + fold(w[0] * u[0] + w[1] * u[1] + w[2] * u[2])
            lo = (g[1], g[2], f[0])
            if i == 0:
                send(j + 1, EARLY)
        ZS[j + 1] = slab
        send(j + 1, LATE)
        MOM[pl.ds(2 * j + 1, 1), :] = jnp.sum(wu, axis=0, keepdims=True)
        MOM[pl.ds(2 * j + 2, 1), :] = jnp.sum(uv, axis=0, keepdims=True)
        return carry

    last = ITERS - 1
    lax.fori_loop(0, last, one_round, 0)

    core = lax.rem(gz, 2)
    group_a = [
        (dx, 0, 0 if dc == 0 else 1 - 2 * core)
        for dx in range(nx)
        for dc in range(2)
        if (dx, dc) != (0, 0)
    ]
    group_b = [(0, dy, dz) for dy in range(ny) for dz in range(0, nz, 2) if (dy, dz) != (0, 0)]

    def spread(n, group, base, into):
        copies = [
            remote(SUM.at[n], into.at[k], a_send.at[base + k], a_recv.at[base + k], offset)
            for k, offset in enumerate(group)
        ]
        for c in copies:
            c.start()
        return copies

    def gather(n, copies, group, base, into):
        for c in copies:
            c.wait_recv()
        return SUM[n] + jnp.sum(into[base : base + len(group)], axis=0)

    n_a, n_b = len(group_a), len(group_b)
    SUM[0] = lanes_of(MOM[...])
    copies_0 = spread(0, group_a, 0, RA)

    receive(last, (9, 11, 5))
    rows_above(last)
    high = ZR[last, 1]
    au = jnp.zeros((8, LANES), F32)
    for i in range(NB):
        ends = [roll(high, 127 - place(f, i) - 1, 1) for f in (0, 1, 3)]
        c, u = fluxes(last, i, ends)
        g = [K[n, i] * c[n] for n in range(3)]
        f = [M[n, i] * u[n] for n in range(3)]
        for n in range(3):
            U[last, n, i] = u[n]
            G[n, i], G[3 + n, i] = g[n], f[n]
        au = au + fold(
            (g[0] * c[0] + g[1] * c[1] + g[2] * c[2]) + (f[0] * u[0] + f[1] * u[1] + f[2] * u[2])
        )
    au = jnp.sum(jnp.sum(au, axis=0, keepdims=True), axis=1, keepdims=True)
    SUM[1] = jnp.broadcast_to(au, (1, LANES))
    copies_1 = spread(1, group_a, n_a, RA2)
    SUM[2] = gather(0, copies_0, group_a, 0, RA)
    copies_2 = spread(2, group_b, 2 * n_a, RB)
    receive(last, (0, 1, 2, 3, 6, 7, 8, 10, 4))
    slabs = edges(last)
    scale = 2.0 / SIGMA

    def last_planes(planes):
        for i in planes:
            if i == 0:
                lo = fluxes_low(last)
            else:
                lo = (G[1, i - 1], G[2, i - 1], G[3, i - 1])
            ends = halo(slabs[0:2], i)
            w = operator(i, [G[n, i] for n in range(3)], [G[3 + n, i] for n in range(3)], lo, ends)
            for n in range(3):
                V[last + 1, n, i] = scale * (w[n] - THETA * V[last, n, i]) - V[last - 1, n, i]

    last_planes(range(0, NB))
    SUM[3] = gather(1, copies_1, group_a, 0, RA2)
    copies_3 = spread(3, group_b, 2 * n_a + n_b, RB2)
    total = gather(2, copies_2, group_b, 0, RB)
    moment = [
        jnp.broadcast_to(jnp.sum(jnp.where(lane_id(1) == m, total, 0.0), axis=1, keepdims=True), (1, LANES))
        for m in range(2 * ITERS - 1)
    ]
    nu = moment[0:2]
    for m in range(2, 2 * ITERS - 1):
        nu.append(2.0 * moment[m] - nu[m % 2])
    cx, cp, cr, ca, gamma, slack, weight = cheb_coefficients(nu)
    for c in range(3):
        for i in range(NB):
            u = [U[j, c, i] for j in range(ITERS)]
            v = [V[j, c, i] for j in range(ITERS + 1)]
            x_out[c, i] = sum(cx[j] * u[j] for j in range(1, last)) + cx[0] * u[0]
            p_out[c, i] = sum(cp[j] * u[j] for j in range(1, ITERS)) + cp[0] * u[0]
            r_out[c, i] = sum(cr[j] * v[j] for j in range(1, ITERS)) + cr[0] * v[0]
            a_out[c, i] = sum(ca[j] * v[j] for j in range(1, ITERS + 1)) + ca[0] * v[0]

    def sent(j, carry):
        for c in messages(j, range(12)):
            c.wait_send()
        return carry

    lax.fori_loop(0, ITERS, sent, 0)
    for c in coef + copies_0 + copies_1 + copies_2 + copies_3:
        c.wait_send()
    au = gather(3, copies_3, group_b, 0, RB2)
    top = scale * (au - THETA * moment[2 * last]) - moment[2 * last - 1]
    alpha_out[...] = gamma / (slack + weight * (2.0 * top - nu[1]))


def body(sizes, right_side, mass_coef, curl_coef):
    shape = right_side.shape
    nx, ny, nz = sizes
    n_a = 2 * nx - 1
    n_b = ny * nz // 2 - 1
    vm = lambda *s: pltpu.VMEM(s, F32)
    dma = lambda *s: pltpu.SemaphoreType.DMA(s)
    x, p, r, a, alpha = pl.pallas_call(
        functools.partial(kernel, sizes),
        out_shape=(pltpu.VMEM(shape, F32),) * 4 + (pltpu.VMEM((1, LANES), F32),),
        in_specs=[pl.BlockSpec(memory_space=pl.ANY)] * 3,
        out_specs=[pl.BlockSpec(memory_space=pltpu.VMEM)] * 5,
        scratch_shapes=[
            vm(5, *shape),
            vm(*shape),
            vm(*shape),
            vm(*shape),
            vm(*shape[1:]),
            vm(4, 4, 10, 48, LANES),
            vm(4, *shape),
            vm(6, *shape[1:]),
            vm(4, ROWS, LANES),
            vm(4, ROWS, LANES),
            vm(4, 8, LANES),
            vm(4, 8, LANES),
            vm(ROWS, LANES),
            vm(ROWS, LANES),
            vm(3, ROWS, LANES),
            vm(4, 7, 8, LANES),
            vm(4, 7, 8, LANES),
            vm(4, ROWS, LANES),
            vm(4, 2, ROWS, LANES),
            vm(4, 4, 8, LANES),
            vm(4, 6, 8, LANES),
            vm(3, 8, LANES),
            vm(*shape[1:]),
            vm(8, LANES),
            vm(4, 1, LANES),
            vm(n_a, 1, LANES),
            vm(n_a, 1, LANES),
            vm(n_b, 1, LANES),
            vm(n_b, 1, LANES),
            dma(6),
            dma(3),
            dma(3),
            dma(4, 12),
            dma(4, 12),
            dma(2 * (n_a + n_b)),
            dma(2 * (n_a + n_b)),
        ],
        compiler_params=pltpu.CompilerParams(collective_id=0, has_side_effects=True),
    )(right_side, mass_coef, curl_coef)
    step = jnp.broadcast_to(alpha[0], shape)
    return x + step * p, r - step * a


def solution(mesh):
    sizes = (mesh.shape["gx"], mesh.shape["gy"], mesh.shape["gz"])
    spec = P(None, "gx", "gy", "gz")
    return jax.shard_map(
        functools.partial(body, sizes),
        mesh=mesh,
        in_specs=(spec,) * 3,
        out_specs=(spec,) * 2,
        check_vma=False,
    )
```

```python
import functools
import jax
import jax.numpy as jnp
from jax import lax
from jax.experimental import pallas as pl
from jax.experimental.pallas import tpu as pltpu
from jax.sharding import PartitionSpec as P

ITERS = 4
THETA = 1.25
SIGMA = 1.25
MESH = pl.DeviceIdType.MESH
F32 = jnp.float32
NB = 8
ROWS = 32
LANES = 128
BASE = 8

ROUND = (
    (1, -1, 0),
    (-1, 1, 0),
    (1, 0, -1),
    (-1, 0, 1),
    (1, 0, 0),
    (-1, 0, 0),
    (0, 1, -1),
    (0, -1, 1),
    (0, 1, 0),
    (0, -1, 0),
    (0, 0, 1),
    (0, 0, -1),
)
UP = (2, 0, 4)
DOWN = (3, 1, 5)
LATE = (6, 7, 8, 9, 10, 11)
FACES = ((1, 0, 0), (-1, 0, 0), (0, 1, 0), (0, -1, 0), (0, 0, 1), (0, 0, -1))
ORDER = (7, 0, 1, 2, 3, 4, 5, 6)


def lane_id(rows=ROWS):
    return lax.broadcasted_iota(jnp.int32, (rows, LANES), 1)


def row_id(rows=ROWS):
    return lax.broadcasted_iota(jnp.int32, (rows, LANES), 0)


def roll(v, amount, axis):
    amount = amount % v.shape[axis]
    return v if amount == 0 else pltpu.roll(v, amount, axis)


def place(field, plane):
    return 16 * field + 2 * plane


def packed(acc, v, field, plane):
    at = place(field, plane)
    return jnp.where((lane_id() >> 1) == at // 2, roll(v, at - 127, 1), acc)


def below_y(v, row):
    return jnp.where(row_id() == 0, row, roll(v, 1, 0))


def first_lane(halo, v):
    return jnp.where(lane_id() == 0, halo, v)


def last_lane(halo, v):
    return jnp.where(lane_id() == 127, halo, v)


def lanes_of(parts):
    sums = jnp.sum(parts, axis=1, keepdims=True)
    return jnp.sum(jnp.where(lane_id(8) == row_id(8), sums, 0.0), axis=0, keepdims=True)


def to_lanes(v, lane):
    out = jnp.zeros((8, LANES), F32)
    for b in range(4):
        out = jnp.where(lane_id(8) == b, roll(v[8 * b : 8 * b + 8], b - lane, 1), out)
    return out


def from_lanes(v, lane):
    return jnp.concatenate([roll(v, lane - b, 1) for b in range(4)], axis=0)


def fold(v):
    return v[0:8] + v[8:16] + v[16:24] + v[24:32]


def cheb_coefficients(nu):
    zero = jnp.zeros_like(nu[0])
    top = 2 * ITERS - 1

    def gram(i, j):
        if i + j == top:
            return 0.5 * nu[abs(i - j)]
        return 0.5 * (nu[i + j] + nu[abs(i - j)])

    def applied(c):
        out = [zero] * (len(c) + 1)
        for i, a in enumerate(c):
            if i == 0:
                out[1] = out[1] + a
            else:
                out[i + 1] = out[i + 1] + 0.5 * a
                out[i - 1] = out[i - 1] + 0.5 * a
        out = [SIGMA * a for a in out]
        for i, a in enumerate(c):
            out[i] = out[i] + THETA * a
        return out

    def dot(c, d):
        total = zero
        for i, a in enumerate(c):
            for j, b in enumerate(d):
                total = total + a * b * gram(i, j)
        return total

    res = [zero + 1.0]
    direction = None
    iterate = [zero] * ITERS
    gamma_old = alpha_old = None
    for iteration in range(ITERS):
        gamma = dot(res, res)
        image = applied(res)
        delta = dot(image, res)
        if iteration == 0:
            alpha = gamma / delta
            direction = list(res)
        else:
            beta = gamma / gamma_old
            slack = delta - beta * gamma / alpha_old
            direction = [
                a + (beta * direction[i] if i < len(direction) else zero) for i, a in enumerate(res)
            ]
            if iteration == ITERS - 1:
                return iterate, direction, res, applied(direction), gamma, slack, 0.5 * image[-1] * res[-1]
            alpha = gamma / slack
        for i, a in enumerate(direction):
            iterate[i] = iterate[i] + alpha * a
        step = applied(direction)
        res = [(res[i] if i < len(res) else zero) - alpha * a for i, a in enumerate(step)]
        gamma_old, alpha_old = gamma, alpha


def kernel(
    sizes,
    r_hbm,
    m_hbm,
    k_hbm,
    x_out,
    p_out,
    r_out,
    a_out,
    alpha_out,
    V,
    M,
    K,
    ID,
    IDN,
    F,
    U,
    G,
    S,
    T,
    XS,
    CX,
    CYS,
    CY,
    CZS,
    CZ,
    CZR,
    YS,
    YR,
    ZS,
    ZR,
    DS,
    DR,
    LOW,
    DN,
    MOM,
    SUM,
    RA,
    RB,
    RC,
    RD,
    load_sem,
    c_send,
    c_recv,
    n_send,
    n_recv,
    a_send,
    a_recv,
):
    nx, ny, nz = sizes
    gx, gy, gz = lax.axis_index("gx"), lax.axis_index("gy"), lax.axis_index("gz")

    def device(dx, dy, dz):
        return {
            "gx": lax.rem(gx + dx + nx, nx),
            "gy": lax.rem(gy + dy + ny, ny),
            "gz": lax.rem(gz + dz + nz, nz),
        }

    def remote(src, dst, send, recv, offset):
        return pltpu.make_async_remote_copy(
            src_ref=src,
            dst_ref=dst,
            send_sem=send,
            recv_sem=recv,
            device_id=device(*offset),
            device_id_type=MESH,
        )

    loads = [
        pltpu.make_async_copy(k_hbm, K, load_sem.at[0]),
        pltpu.make_async_copy(m_hbm, M, load_sem.at[1]),
        pltpu.make_async_copy(r_hbm, V.at[0], load_sem.at[2]),
    ]
    first = [
        pltpu.make_async_copy(k_hbm.at[1:3, NB - 1], XS.at[0:2], load_sem.at[3]),
        pltpu.make_async_copy(m_hbm.at[0, NB - 1], XS.at[2], load_sem.at[4]),
        pltpu.make_async_copy(r_hbm.at[0, NB - 1], XS.at[3], load_sem.at[5]),
    ]
    for c in first:
        c.start()
    for c in loads:
        c.start()
    barrier = pltpu.get_barrier_semaphore()
    for o in FACES:
        pl.semaphore_signal(barrier, inc=1, device_id=device(*o), device_id_type=MESH)
    coef = [
        remote(XS, CX, c_send.at[0], c_recv.at[0], (1, 0, 0)),
        remote(CYS, CY, c_send.at[1], c_recv.at[1], (0, 1, 0)),
        remote(CZS, CZ, c_send.at[2], c_recv.at[2], (0, 0, 1)),
    ]
    for c in first:
        c.wait()
    pl.semaphore_wait(barrier, len(FACES))
    coef[0].start()
    for c in loads:
        c.wait()
    y_fields = (K.at[0], K.at[2], M.at[1], V.at[0, 1])
    z_fields = (K.at[0], K.at[1], M.at[2], V.at[0, 2])
    for f, ref in enumerate(y_fields):
        for i in range(NB):
            CYS[f, i : i + 1, :] = ref[i, 31:32, :]
    coef[1].start()
    slab = jnp.zeros((ROWS, LANES), F32)
    for f, ref in enumerate(z_fields):
        for i in range(NB):
            slab = packed(slab, ref[i], f, i)
    CZS[...] = slab
    coef[2].start()
    for i in range(NB):
        S[0, i] = roll(K[0, i], 1, 1)
        S[1, i] = roll(K[1, i], 1, 1)
        S[2, i] = roll(M[2, i], 1, 1)
        S[3, i] = roll(V[0, 2, i], 1, 1)
    for c in coef:
        c.wait_recv()

    def messages(j, which):
        pairs = (
            (DS.at[j, 0], DR.at[j, 0]),
            (DS.at[j, 1], DR.at[j, 1]),
            (DS.at[j, 2], DR.at[j, 2]),
            (DS.at[j, 3], DR.at[j, 3]),
            (F.at[j, 0:4, NB, BASE : BASE + ROWS], F.at[j, 0:4, 0, BASE : BASE + ROWS]),
            (F.at[j, 1:4, 1, BASE : BASE + ROWS], F.at[j, 1:4, NB + 1, BASE : BASE + ROWS]),
            (YS.at[j, 1], DR.at[j, 4]),
            (ZS.at[j, 0:8], DR.at[j, 5]),
            (YS.at[j, 0:4], YR.at[j, 0:4]),
            (YS.at[j, 4:7], YR.at[j, 4:7]),
            (ZS.at[j], ZR.at[j, 0]),
            (ZS.at[j], ZR.at[j, 1]),
        )
        return [
            remote(*pairs[k], n_send.at[j, k], n_recv.at[j, k], ROUND[k]) for k in which
        ]

    def send(j, which):
        for c in messages(j, which):
            c.start()

    def receive(j, which):
        for c in messages(j, which):
            c.wait_recv()

    def finish(j, i, slab, values):
        for f, v in enumerate(values):
            F[j, f, 1 + i, BASE : BASE + ROWS, :] = v
            YS[j, f, i : i + 1, :] = v[31:32]
            if f != 1:
                YS[j, (4, 0, 5, 6)[f], i : i + 1, :] = v[0:1]
            slab = packed(slab, v, f, i)
        if i == NB - 1:
            DS[j, 0] = jnp.broadcast_to(values[0][0:1], (8, LANES))
            DS[j, 2] = to_lanes(values[0], 0)
        if i == 0:
            DS[j, 1] = jnp.broadcast_to(values[1][31:32], (8, LANES))
            DS[j, 3] = to_lanes(values[2], 127)
        return slab

    slab = jnp.zeros((ROWS, LANES), F32)
    cz = CZ[...]
    for f in range(3):
        CZR[f] = roll(cz, 2 - 16 * f, 1)
    for i in ORDER:
        k0, k1, k2 = K[0, i], K[1, i], K[2, i]
        m0, m1, m2 = M[0, i], M[1, i], M[2, i]
        r0, r1, r2 = V[0, 0, i], V[0, 1, i], V[0, 2, i]
        if i == 0:
            k1_lo, k2_lo, m0_lo, r0_lo = CX[0], CX[1], CX[2], CX[3]
        else:
            k1_lo, k2_lo, m0_lo, r0_lo = K[1, i - 1], K[2, i - 1], M[0, i - 1], V[0, 0, i - 1]
        k0y = below_y(k0, CY[0, i : i + 1, :])
        k2y = below_y(k2, CY[1, i : i + 1, :])
        m1y = below_y(m1, CY[2, i : i + 1, :])
        r1y = below_y(r1, CY[3, i : i + 1, :])
        k0z = first_lane(roll(cz, -place(0, i), 1), S[0, i])
        k1z = first_lane(roll(cz, -place(1, i), 1), S[1, i])
        m2z = first_lane(roll(cz, -place(2, i), 1), S[2, i])
        r2z = first_lane(roll(cz, -place(3, i), 1), S[3, i])
        id0 = 1.0 / (m0 + k1 + k1z + k2 + k2y)
        id1 = 1.0 / (m1 + k2 + k2_lo + k0 + k0z)
        id2 = 1.0 / (m2 + k0 + k0y + k1 + k1_lo)
        dn = m0 + m0_lo + m1 + m1y + m2 + m2z
        idn = 1.0 / dn
        phi = idn * ((r0_lo - r0) + (r1y - r1) + (r2z - r2))
        ID[0, i], ID[1, i], ID[2, i], IDN[i], DN[i] = id0, id1, id2, idn, dn
        s0, s1, s2 = r0 * id0, r1 * id1, r2 * id2
        slab = finish(0, i, slab, (s0, s1, s2, phi))
        if i == 7:
            send(0, UP)
        if i == 0:
            send(0, DOWN)
    ZS[0] = slab
    send(0, LATE)
    MOM[7:8, :] = jnp.zeros((1, LANES), F32)

    def field(j, f, i):
        return F[j, f, 1 + i, BASE : BASE + ROWS, :]

    def above_y(j, f, i):
        return F[j, f, 1 + i, BASE + 1 : BASE + 1 + ROWS, :]

    def rows_above(j):
        for f, at in ((0, 4), (2, 5), (3, 6)):
            for i in range(NB):
                F[j, f, 1 + i, BASE + ROWS : BASE + ROWS + 1, :] = YR[j, at, i : i + 1, :]

    def edges(j):
        F[j, 0, 0, BASE + ROWS : BASE + ROWS + 1, :] = DR[j, 0, 0:1, :]
        sub, lane8 = row_id(8), lane_id(8)
        s0, s1, s2, ph = YR[j, 0], YR[j, 1], YR[j, 2], YR[j, 3]
        own0, own2, own_ph = YS[j, 4], YS[j, 5], YS[j, 6]
        s1x = jnp.where(sub == 7, DR[j, 1], roll(s1, -1, 0))
        s1z = jnp.where(lane8 == 127, roll(DR[j, 4], -1, 1), roll(s1, -1, 1))
        LOW[0] = CY[0] * ((own2 - s2) - (s1z - s1))
        LOW[1] = CY[1] * ((s1x - s1) - (own0 - s0))
        LOW[2] = CY[2] * (s1 + (own_ph - ph))
        lane, row = lane_id(), row_id()
        low = jnp.where((lane & 1) == 1, ZS[j], ZR[j, 0])
        z0, z1, z2, zp = (roll(low, 2 - 16 * f, 1) for f in range(4))
        z2y = jnp.where(row == 31, roll(DR[j, 5], 2 - 32, 1)[0:1], roll(z2, -1, 0))
        z2x = jnp.where(lane == 16, from_lanes(DR[j, 3], 16), roll(z2, -2, 1))
        gz0 = CZR[0] * ((z2y - z2) - (roll(z1, -1, 1) - z1))
        gz1 = CZR[1] * ((roll(z0, -1, 1) - z0) - (z2x - z2))
        mz2 = CZR[2] * (z2 + (roll(zp, -1, 1) - zp))
        odd = (lane & 1) == 1
        high = ZR[j, 1]
        return (
            jnp.where(odd, high, gz1),
            jnp.where(odd, roll(high, -16, 1), gz0),
            jnp.where(odd, roll(high, -48, 1), mz2),
        )

    def ahead(j):
        first = j == 0
        scale = jnp.where(first, F32(1.0 / SIGMA), F32(2.0 / SIGMA))
        back = jnp.where(first, F32(0.0), F32(1.0))
        before = jnp.maximum(j - 1, 0)
        uv = jnp.zeros((8, LANES), F32)
        for i in range(NB):
            e0, e1, e2, ph = (field(j, f, i) for f in range(4))
            v = [V[j, n, i] for n in range(3)]
            e0z, e1z, phz = roll(e0, -1, 1), roll(e1, -1, 1), roll(ph, -1, 1)
            S[0, i], S[1, i], S[2, i] = e0z, e1z, phz
            c0 = (above_y(j, 2, i) - e2) - (e1z - e1)
            S[3, i] = roll(K[0, i] * c0, 1, 1)
            if i < NB - 1:
                S[4, i] = roll(K[1, i] * ((e0z - e0) - (field(j, 2, i + 1) - e2)), 1, 1)
            S[5, i] = roll(M[2, i] * (e2 + (phz - ph)), 1, 1)
            for n in range(3):
                T[n, i] = (scale * THETA) * v[n] + back * V[before, n, i]
            T[3, i] = (scale * THETA) * ph + back * field(before, 3, i)
            uv = uv + fold(v[0] * e0 + v[1] * e1 + v[2] * e2 + DN[i] * ph * ph)
        MOM[pl.ds(2 * j, 1), :] = jnp.sum(uv, axis=0, keepdims=True)

    def halo(slabs, i):
        return [roll(t, 126 - 2 * i, 1) for t in slabs]

    def fluxes_low(j):
        e0, e1, e2, ph = (field(j, f, -1) for f in range(4))
        n1, n2, nph = (field(j, f, 0) for f in (1, 2, 3))
        e0z = jnp.where(lane_id() == 127, from_lanes(DR[j, 2], 127), roll(e0, -1, 1))
        g1 = CX[0] * ((e0z - e0) - (n2 - e2))
        g2 = CX[1] * ((n1 - e1) - (above_y(j, 0, -1) - e0))
        return g1, g2, CX[2] * (e0 + (nph - ph))

    def fluxes_before(j, i, slabs):
        e0, e1, e2, ph = (field(j, f, i) for f in range(4))
        n1, n2, nph = (field(j, f, i + 1) for f in (1, 2, 3))
        e0z = last_lane(roll(slabs[0], 126 - 2 * i, 1), S[0, i])
        g1 = K[1, i] * ((e0z - e0) - (n2 - e2))
        g2 = K[2, i] * ((n1 - e1) - (above_y(j, 0, i) - e0))
        return g1, g2, M[0, i] * (e0 + (nph - ph))

    def fluxes(j, i, ends):
        e0, e1, e2, ph = (field(j, f, i) for f in range(4))
        n1, n2, nph = (field(j, f, i + 1) for f in (1, 2, 3))
        e0z = last_lane(ends[0], S[0, i])
        e1z = last_lane(ends[1], S[1, i])
        phz = last_lane(ends[2], S[2, i])
        c0 = (above_y(j, 2, i) - e2) - (e1z - e1)
        c1 = (e0z - e0) - (n2 - e2)
        c2 = (n1 - e1) - (above_y(j, 0, i) - e0)
        u0 = e0 + (nph - ph)
        u1 = e1 + (above_y(j, 3, i) - ph)
        u2 = e2 + (phz - ph)
        return (c0, c1, c2), (u0, u1, u2)

    def operator(i, g, f, lo, ends):
        g0, g1, g2 = g
        f0, f1, f2 = f
        g1_lo, g2_lo, f0_lo = lo
        g0y = below_y(g0, LOW[0, i : i + 1, :])
        g2y = below_y(g2, LOW[1, i : i + 1, :])
        g0z = jnp.concatenate([S[3, i, 0:24], roll(g0[24:32], 1, 1)], axis=0)
        g0z = first_lane(ends[1], g0z)
        g1z = first_lane(ends[0], roll(g1, 1, 1) if i == NB - 1 else S[4, i])
        w0 = (g1z - g1) - (g2y - g2) + f0
        w1 = (g2_lo - g2) - (g0z - g0) + f1
        w2 = (g0y - g0) - (g1_lo - g1) + f2
        return w0, w1, w2

    def divergence(i, f, lo, ends):
        f1y = below_y(f[1], LOW[2, i : i + 1, :])
        f2z = first_lane(ends[2], S[5, i])
        return IDN[i] * ((lo[2] - f[0]) + (f1y - f[1]) + (f2z - f[2]))

    def one_round(j, carry):
        receive(j, (0, 1, 2, 3, 6, 7, 8, 9, 10, 11, 4, 5))
        scale = jnp.where(j == 0, F32(1.0 / SIGMA), F32(2.0 / SIGMA))
        rows_above(j)
        slabs = edges(j)
        slab = jnp.zeros((ROWS, LANES), F32)
        for i in ORDER:
            if i == 7:
                lo = fluxes_before(j, 6, slabs)
            if i == 0:
                lo = fluxes_low(j)
            ends = halo(slabs, i)
            c, u = fluxes(j, i, ends)
            g = [K[n, i] * c[n] for n in range(3)]
            f = [M[n, i] * u[n] for n in range(3)]
            w = operator(i, g, f, lo, ends)
            q = divergence(i, f, lo, ends)
            w = [scale * w[n] - T[n, i] for n in range(3)]
            q = scale * q - T[3, i]
            for n in range(3):
                U[j, n, i] = u[n]
                V[j + 1, n, i] = w[n]
            s = [w[n] * ID[n, i] for n in range(3)]
            slab = finish(j + 1, i, slab, s + [q])
            lo = (g[1], g[2], f[0])
            if i == 7:
                send(j + 1, UP)
            if i == 0:
                send(j + 1, DOWN)
        ZS[j + 1] = slab
        send(j + 1, LATE)
        ahead(j + 1)
        wu = jnp.zeros((8, LANES), F32)
        for i in range(NB):
            w = [V[j + 1, n, i] for n in range(3)]
            wu = wu + fold(w[0] * U[j, 0, i] + w[1] * U[j, 1, i] + w[2] * U[j, 2, i])
        MOM[pl.ds(2 * j + 1, 1), :] = jnp.sum(wu, axis=0, keepdims=True)
        return carry

    last = ITERS - 1
    ahead(0)
    lax.fori_loop(0, last, one_round, 0)

    core = lax.rem(gz, 2)
    group_a = [
        (dx, 0, 0 if dc == 0 else 1 - 2 * core)
        for dx in range(nx)
        for dc in range(2)
        if (dx, dc) != (0, 0)
    ]
    pair = [(0, 0, 1 - 2 * core)]
    chips = [
        (dx, dy, dz)
        for dx in range(nx)
        for dy in range(ny)
        for dz in range(0, nz, 2)
        if (dx, dy, dz) != (0, 0, 0)
    ]
    group_b = [(0, dy, dz) for dy in range(ny) for dz in range(0, nz, 2) if (dy, dz) != (0, 0)]

    def spread(n, group, base, into):
        copies = [
            remote(SUM.at[n], into.at[k], a_send.at[base + k], a_recv.at[base + k], offset)
            for k, offset in enumerate(group)
        ]
        for c in copies:
            c.start()
        return copies

    def gather(n, copies, group, base, into):
        for c in copies:
            c.wait_recv()
        return SUM[n] + jnp.sum(into[base : base + len(group)], axis=0)

    n_a, n_b = len(group_a), len(group_b)
    SUM[0] = lanes_of(MOM[...])
    copies_0 = spread(0, group_a, 0, RA)

    receive(last, (9, 11, 5))
    rows_above(last)
    high = ZR[last, 1]
    au = jnp.zeros((8, LANES), F32)
    for i in range(NB):
        ends = [roll(high, 127 - place(f, i) - 1, 1) for f in (0, 1, 3)]
        c, u = fluxes(last, i, ends)
        g = [K[n, i] * c[n] for n in range(3)]
        f = [M[n, i] * u[n] for n in range(3)]
        for n in range(3):
            U[last, n, i] = u[n]
            G[n, i], G[3 + n, i] = g[n], f[n]
        au = au + fold(
            (g[0] * c[0] + g[1] * c[1] + g[2] * c[2]) + (f[0] * u[0] + f[1] * u[1] + f[2] * u[2])
        )
    au = jnp.sum(jnp.sum(au, axis=0, keepdims=True), axis=1, keepdims=True)
    SUM[1] = jnp.broadcast_to(au, (1, LANES))
    copies_1 = spread(1, pair, n_a + n_b, RC)
    SUM[3] = gather(1, copies_1, pair, 0, RC)
    copies_3 = spread(3, chips, n_a + n_b + 1, RD)
    SUM[2] = gather(0, copies_0, group_a, 0, RA)
    copies_2 = spread(2, group_b, n_a, RB)
    receive(last, (0, 1, 2, 3, 6, 7, 8, 10, 4))
    slabs = edges(last)
    scale = 2.0 / SIGMA

    def last_planes(planes):
        for i in planes:
            if i == 0:
                lo = fluxes_low(last)
            else:
                lo = (G[1, i - 1], G[2, i - 1], G[3, i - 1])
            ends = halo(slabs[0:2], i)
            w = operator(i, [G[n, i] for n in range(3)], [G[3 + n, i] for n in range(3)], lo, ends)
            for n in range(3):
                V[last + 1, n, i] = scale * w[n] - T[n, i]

    last_planes(range(0, NB))
    total = gather(2, copies_2, group_b, 0, RB)
    moment = [
        jnp.broadcast_to(jnp.sum(jnp.where(lane_id(1) == m, total, 0.0), axis=1, keepdims=True), (1, LANES))
        for m in range(2 * ITERS - 1)
    ]
    nu = moment[0:2]
    for m in range(2, 2 * ITERS - 1):
        nu.append(2.0 * moment[m] - nu[m % 2])
    cx, cp, cr, ca, gamma, slack, weight = cheb_coefficients(nu)
    for c in range(3):
        for i in range(NB):
            u = [U[j, c, i] for j in range(ITERS)]
            v = [V[j, c, i] for j in range(ITERS + 1)]
            x_out[c, i] = sum(cx[j] * u[j] for j in range(1, last)) + cx[0] * u[0]
            p_out[c, i] = sum(cp[j] * u[j] for j in range(1, ITERS)) + cp[0] * u[0]
            r_out[c, i] = sum(cr[j] * v[j] for j in range(1, ITERS)) + cr[0] * v[0]
            a_out[c, i] = sum(ca[j] * v[j] for j in range(1, ITERS + 1)) + ca[0] * v[0]

    def sent(j, carry):
        for c in messages(j, range(12)):
            c.wait_send()
        return carry

    lax.fori_loop(0, ITERS, sent, 0)
    for c in coef + copies_0 + copies_1 + copies_2 + copies_3:
        c.wait_send()
    au = gather(3, copies_3, chips, 0, RD)
    top = scale * (au - THETA * moment[2 * last]) - moment[2 * last - 1]
    alpha_out[...] = gamma / (slack + weight * (2.0 * top - nu[1]))


def body(sizes, right_side, mass_coef, curl_coef):
    shape = right_side.shape
    nx, ny, nz = sizes
    n_a = 2 * nx - 1
    n_b = ny * nz // 2 - 1
    n_c = nx * ny * nz // 2 - 1
    vm = lambda *s: pltpu.VMEM(s, F32)
    dma = lambda *s: pltpu.SemaphoreType.DMA(s)
    x, p, r, a, alpha = pl.pallas_call(
        functools.partial(kernel, sizes),
        out_shape=(pltpu.VMEM(shape, F32),) * 4 + (pltpu.VMEM((1, LANES), F32),),
        in_specs=[pl.BlockSpec(memory_space=pl.ANY)] * 3,
        out_specs=[pl.BlockSpec(memory_space=pltpu.VMEM)] * 5,
        scratch_shapes=[
            vm(5, *shape),
            vm(*shape),
            vm(*shape),
            vm(*shape),
            vm(*shape[1:]),
            vm(4, 4, 10, 48, LANES),
            vm(4, *shape),
            vm(6, *shape[1:]),
            vm(6, *shape[1:]),
            vm(4, *shape[1:]),
            vm(4, ROWS, LANES),
            vm(4, ROWS, LANES),
            vm(4, 8, LANES),
            vm(4, 8, LANES),
            vm(ROWS, LANES),
            vm(ROWS, LANES),
            vm(3, ROWS, LANES),
            vm(4, 7, 8, LANES),
            vm(4, 7, 8, LANES),
            vm(4, ROWS, LANES),
            vm(4, 2, ROWS, LANES),
            vm(4, 4, 8, LANES),
            vm(4, 6, 8, LANES),
            vm(3, 8, LANES),
            vm(*shape[1:]),
            vm(8, LANES),
            vm(4, 1, LANES),
            vm(n_a, 1, LANES),
            vm(n_b, 1, LANES),
            vm(1, 1, LANES),
            vm(n_c, 1, LANES),
            dma(6),
            dma(3),
            dma(3),
            dma(4, 12),
            dma(4, 12),
            dma(n_a + n_b + 1 + n_c),
            dma(n_a + n_b + 1 + n_c),
        ],
        compiler_params=pltpu.CompilerParams(collective_id=0, has_side_effects=True),
    )(right_side, mass_coef, curl_coef)
    step = jnp.broadcast_to(alpha[0], shape)
    return x + step * p, r - step * a


def solution(mesh):
    sizes = (mesh.shape["gx"], mesh.shape["gy"], mesh.shape["gz"])
    spec = P(None, "gx", "gy", "gz")
    return jax.shard_map(
        functools.partial(body, sizes),
        mesh=mesh,
        in_specs=(spec,) * 3,
        out_specs=(spec,) * 2,
        check_vma=False,
    )
```

```python
import functools
import jax
import jax.numpy as jnp
from jax import lax
from jax.experimental import pallas as pl
from jax.experimental.pallas import tpu as pltpu
from jax.sharding import PartitionSpec as P

ITERS = 4
THETA = 1.25
SIGMA = 1.25
MESH = pl.DeviceIdType.MESH
F32 = jnp.float32
NB = 8
ROWS = 32
LANES = 128
BASE = 8

ROUND = (
    (1, -1, 0),
    (-1, 1, 0),
    (1, 0, -1),
    (-1, 0, 1),
    (1, 0, 0),
    (-1, 0, 0),
    (0, 1, -1),
    (0, -1, 1),
    (0, 1, 0),
    (0, -1, 0),
    (0, 0, 1),
    (0, 0, -1),
)
UP = (2, 0, 4)
DOWN = (3, 1, 5)
LATE = (6, 7, 8, 9, 10, 11)
FACES = ((1, 0, 0), (-1, 0, 0), (0, 1, 0), (0, -1, 0), (0, 0, 1), (0, 0, -1))
START = (7, 6, 5, 4, 3, 2, 1, 0)


def lane_id(rows=ROWS):
    return lax.broadcasted_iota(jnp.int32, (rows, LANES), 1)


def row_id(rows=ROWS):
    return lax.broadcasted_iota(jnp.int32, (rows, LANES), 0)


def roll(v, amount, axis):
    amount = amount % v.shape[axis]
    return v if amount == 0 else pltpu.roll(v, amount, axis)


def place(field, plane):
    return 16 * field + 2 * plane


def packed(acc, v, field, plane):
    at = place(field, plane)
    return jnp.where((lane_id() >> 1) == at // 2, roll(v, at - 127, 1), acc)


def below_y(v, row):
    return jnp.where(row_id() == 0, row, roll(v, 1, 0))


def first_lane(halo, v):
    return jnp.where(lane_id() == 0, halo, v)


def last_lane(halo, v):
    return jnp.where(lane_id() == 127, halo, v)


def lanes_of(parts):
    sums = jnp.sum(parts, axis=1, keepdims=True)
    return jnp.sum(jnp.where(lane_id(8) == row_id(8), sums, 0.0), axis=0, keepdims=True)


def to_lanes(v, lane):
    out = jnp.zeros((8, LANES), F32)
    for b in range(4):
        out = jnp.where(lane_id(8) == b, roll(v[8 * b : 8 * b + 8], b - lane, 1), out)
    return out


def from_lanes(v, lane):
    return jnp.concatenate([roll(v, lane - b, 1) for b in range(4)], axis=0)


def fold(v):
    return v[0:8] + v[8:16] + v[16:24] + v[24:32]


def cheb_coefficients(nu):
    zero = jnp.zeros_like(nu[0])
    top = 2 * ITERS - 1

    def gram(i, j):
        if i + j == top:
            return 0.5 * nu[abs(i - j)]
        return 0.5 * (nu[i + j] + nu[abs(i - j)])

    def applied(c):
        out = [zero] * (len(c) + 1)
        for i, a in enumerate(c):
            if i == 0:
                out[1] = out[1] + a
            else:
                out[i + 1] = out[i + 1] + 0.5 * a
                out[i - 1] = out[i - 1] + 0.5 * a
        out = [SIGMA * a for a in out]
        for i, a in enumerate(c):
            out[i] = out[i] + THETA * a
        return out

    def dot(c, d):
        total = zero
        for i, a in enumerate(c):
            for j, b in enumerate(d):
                total = total + a * b * gram(i, j)
        return total

    res = [zero + 1.0]
    direction = None
    iterate = [zero] * ITERS
    gamma_old = alpha_old = None
    for iteration in range(ITERS):
        gamma = dot(res, res)
        image = applied(res)
        delta = dot(image, res)
        if iteration == 0:
            alpha = gamma / delta
            direction = list(res)
        else:
            beta = gamma / gamma_old
            slack = delta - beta * gamma / alpha_old
            direction = [
                a + (beta * direction[i] if i < len(direction) else zero) for i, a in enumerate(res)
            ]
            if iteration == ITERS - 1:
                return iterate, direction, res, applied(direction), gamma, slack, 0.5 * image[-1] * res[-1]
            alpha = gamma / slack
        for i, a in enumerate(direction):
            iterate[i] = iterate[i] + alpha * a
        step = applied(direction)
        res = [(res[i] if i < len(res) else zero) - alpha * a for i, a in enumerate(step)]
        gamma_old, alpha_old = gamma, alpha


def kernel(
    sizes,
    r_hbm,
    m_hbm,
    k_hbm,
    x_out,
    p_out,
    r_out,
    a_out,
    alpha_out,
    V,
    M,
    K,
    ID,
    IDN,
    F,
    U,
    G,
    S,
    T,
    XS,
    CX,
    CYS,
    CY,
    CZS,
    CZ,
    CZR,
    CZ7,
    YS,
    YR,
    ZS,
    ZR,
    DS,
    DR,
    LOW,
    DN,
    MOM,
    SUM,
    RA,
    RB,
    RC,
    RD,
    load_sem,
    c_send,
    c_recv,
    n_send,
    n_recv,
    a_send,
    a_recv,
):
    nx, ny, nz = sizes
    gx, gy, gz = lax.axis_index("gx"), lax.axis_index("gy"), lax.axis_index("gz")

    def device(dx, dy, dz):
        return {
            "gx": lax.rem(gx + dx + nx, nx),
            "gy": lax.rem(gy + dy + ny, ny),
            "gz": lax.rem(gz + dz + nz, nz),
        }

    def remote(src, dst, send, recv, offset):
        return pltpu.make_async_remote_copy(
            src_ref=src,
            dst_ref=dst,
            send_sem=send,
            recv_sem=recv,
            device_id=device(*offset),
            device_id_type=MESH,
        )

    loads = [
        pltpu.make_async_copy(k_hbm, K, load_sem.at[0]),
        pltpu.make_async_copy(m_hbm, M, load_sem.at[1]),
        pltpu.make_async_copy(r_hbm, V.at[0], load_sem.at[2]),
    ]
    first = [
        pltpu.make_async_copy(k_hbm.at[1:3, NB - 1], XS.at[0:2], load_sem.at[3]),
        pltpu.make_async_copy(m_hbm.at[0, NB - 1], XS.at[2], load_sem.at[4]),
        pltpu.make_async_copy(r_hbm.at[0, NB - 1], XS.at[3], load_sem.at[5]),
    ]
    for c in first:
        c.start()
    for c in loads:
        c.start()
    barrier = pltpu.get_barrier_semaphore()
    for o in FACES:
        pl.semaphore_signal(barrier, inc=1, device_id=device(*o), device_id_type=MESH)
    coef = [
        remote(XS, CX, c_send.at[0], c_recv.at[0], (1, 0, 0)),
        remote(CYS, CY, c_send.at[1], c_recv.at[1], (0, 1, 0)),
        remote(CZS, CZ, c_send.at[2], c_recv.at[2], (0, 0, 1)),
    ]
    for c in first:
        c.wait()
    pl.semaphore_wait(barrier, len(FACES))
    coef[0].start()
    for c in loads:
        c.wait()
    y_fields = (K.at[0], K.at[2], M.at[1], V.at[0, 1])
    z_fields = (K.at[0], K.at[1], M.at[2], V.at[0, 2])
    for f, ref in enumerate(y_fields):
        for i in range(NB):
            CYS[f, i : i + 1, :] = ref[i, 31:32, :]
    coef[1].start()
    slab = jnp.zeros((ROWS, LANES), F32)
    for f, ref in enumerate(z_fields):
        for i in range(NB):
            slab = packed(slab, ref[i], f, i)
    CZS[...] = slab
    coef[2].start()
    for i in range(NB):
        S[0, i] = roll(K[0, i], 1, 1)
        S[1, i] = roll(K[1, i], 1, 1)
        S[2, i] = roll(M[2, i], 1, 1)
        S[3, i] = roll(V[0, 2, i], 1, 1)
    coef[1].wait_recv()
    coef[2].wait_recv()

    def messages(j, which):
        pairs = (
            (DS.at[j, 0], DR.at[j, 0]),
            (DS.at[j, 1], DR.at[j, 1]),
            (DS.at[j, 2], DR.at[j, 2]),
            (DS.at[j, 3], DR.at[j, 3]),
            (F.at[j, 0:4, NB, BASE : BASE + ROWS], F.at[j, 0:4, 0, BASE : BASE + ROWS]),
            (F.at[j, 1:4, 1, BASE : BASE + ROWS], F.at[j, 1:4, NB + 1, BASE : BASE + ROWS]),
            (YS.at[j, 1], DR.at[j, 4]),
            (ZS.at[j, 0:8], DR.at[j, 5]),
            (YS.at[j, 0:4], YR.at[j, 0:4]),
            (YS.at[j, 4:7], YR.at[j, 4:7]),
            (ZS.at[j], ZR.at[j, 0]),
            (ZS.at[j], ZR.at[j, 1]),
        )
        return [
            remote(*pairs[k], n_send.at[j, k], n_recv.at[j, k], ROUND[k]) for k in which
        ]

    def send(j, which):
        for c in messages(j, which):
            c.start()

    def receive(j, which):
        for c in messages(j, which):
            c.wait_recv()

    def finish(j, i, slab, values):
        for f, v in values.items():
            F[j, f, 1 + i, BASE : BASE + ROWS, :] = v
            YS[j, f, i : i + 1, :] = v[31:32]
            if f != 1:
                YS[j, (4, 0, 5, 6)[f], i : i + 1, :] = v[0:1]
            slab = packed(slab, v, f, i)
        return slab

    def diagonals(j, s0, s1, s2):
        if s0 is not None:
            DS[j, 0] = jnp.broadcast_to(s0[0:1], (8, LANES))
            DS[j, 2] = to_lanes(s0, 0)
        if s1 is not None:
            DS[j, 1] = jnp.broadcast_to(s1[31:32], (8, LANES))
            DS[j, 3] = to_lanes(s2, 127)

    slab = jnp.zeros((ROWS, LANES), F32)
    cz = CZ[...]
    for f in range(3):
        CZR[f] = roll(cz, 2 - 16 * f, 1)
    CZ7[...] = roll(cz, -place(1, NB - 1), 1)
    for i in START:
        if i == 0:
            coef[0].wait_recv()
        k0, k1, k2 = K[0, i], K[1, i], K[2, i]
        m0, m1, m2 = M[0, i], M[1, i], M[2, i]
        r0, r1, r2 = V[0, 0, i], V[0, 1, i], V[0, 2, i]
        if i == 0:
            k1_lo, k2_lo, m0_lo, r0_lo = CX[0], CX[1], CX[2], CX[3]
        else:
            k1_lo, k2_lo, m0_lo, r0_lo = K[1, i - 1], K[2, i - 1], M[0, i - 1], V[0, 0, i - 1]
        k0y = below_y(k0, CY[0, i : i + 1, :])
        k2y = below_y(k2, CY[1, i : i + 1, :])
        m1y = below_y(m1, CY[2, i : i + 1, :])
        r1y = below_y(r1, CY[3, i : i + 1, :])
        k0z = first_lane(roll(cz, -place(0, i), 1), S[0, i])
        k1z = first_lane(roll(cz, -place(1, i), 1), S[1, i])
        m2z = first_lane(roll(cz, -place(2, i), 1), S[2, i])
        r2z = first_lane(roll(cz, -place(3, i), 1), S[3, i])
        id0 = 1.0 / (m0 + k1 + k1z + k2 + k2y)
        id1 = 1.0 / (m1 + k2 + k2_lo + k0 + k0z)
        id2 = 1.0 / (m2 + k0 + k0y + k1 + k1_lo)
        dn = m0 + m0_lo + m1 + m1y + m2 + m2z
        idn = 1.0 / dn
        phi = idn * ((r0_lo - r0) + (r1y - r1) + (r2z - r2))
        ID[0, i], ID[1, i], ID[2, i], IDN[i], DN[i] = id0, id1, id2, idn, dn
        s0, s1, s2 = r0 * id0, r1 * id1, r2 * id2
        slab = finish(0, i, slab, {0: s0, 1: s1, 2: s2, 3: phi})
        diagonals(0, s0 if i == 7 else None, s1 if i == 0 else None, s2)
        if i == 7:
            send(0, UP)
        if i == 0:
            send(0, DOWN)
    ZS[0] = slab
    send(0, LATE)
    MOM[7:8, :] = jnp.zeros((1, LANES), F32)

    def field(j, f, i):
        return F[j, f, 1 + i, BASE : BASE + ROWS, :]

    def above_y(j, f, i):
        return F[j, f, 1 + i, BASE + 1 : BASE + 1 + ROWS, :]

    def rows_above(j):
        for f, at in ((0, 4), (2, 5), (3, 6)):
            for i in range(NB):
                F[j, f, 1 + i, BASE + ROWS : BASE + ROWS + 1, :] = YR[j, at, i : i + 1, :]

    def edges(j, diag):
        sub, lane8 = row_id(8), lane_id(8)
        s0, s1, s2, ph = YR[j, 0], YR[j, 1], YR[j, 2], YR[j, 3]
        own0, own2, own_ph = YS[j, 4], YS[j, 5], YS[j, 6]
        s1x = jnp.where(sub == 7, DR[j, 1] if diag else 0.0, roll(s1, -1, 0))
        s1z = jnp.where(lane8 == 127, roll(DR[j, 4], -1, 1), roll(s1, -1, 1))
        LOW[0] = CY[0] * ((own2 - s2) - (s1z - s1))
        LOW[1] = CY[1] * ((s1x - s1) - (own0 - s0))
        LOW[2] = CY[2] * (s1 + (own_ph - ph))
        lane, row = lane_id(), row_id()
        low = jnp.where((lane & 1) == 1, ZS[j], ZR[j, 0])
        z0, z1, z2, zp = (roll(low, 2 - 16 * f, 1) for f in range(4))
        z2y = jnp.where(row == 31, roll(DR[j, 5], 2 - 32, 1)[0:1], roll(z2, -1, 0))
        z2x = jnp.where(lane == 16, from_lanes(DR[j, 3], 16) if diag else 0.0, roll(z2, -2, 1))
        gz0 = CZR[0] * ((z2y - z2) - (roll(z1, -1, 1) - z1))
        gz1 = CZR[1] * ((roll(z0, -1, 1) - z0) - (z2x - z2))
        mz2 = CZR[2] * (z2 + (roll(zp, -1, 1) - zp))
        odd = (lane & 1) == 1
        high = ZR[j, 1]
        return (
            jnp.where(odd, high, gz1),
            jnp.where(odd, roll(high, -16, 1), gz0),
            jnp.where(odd, roll(high, -48, 1), mz2),
        )

    def ahead(j):
        first = j == 0
        scale = jnp.where(first, F32(1.0 / SIGMA), F32(2.0 / SIGMA))
        back = jnp.where(first, F32(0.0), F32(1.0))
        before = jnp.maximum(j - 1, 0)
        uv = jnp.zeros((8, LANES), F32)
        for i in range(NB):
            e0, e1, e2, ph = (field(j, f, i) for f in range(4))
            v = [V[j, n, i] for n in range(3)]
            e0z, e1z, phz = roll(e0, -1, 1), roll(e1, -1, 1), roll(ph, -1, 1)
            S[0, i], S[1, i], S[2, i] = e0z, e1z, phz
            c0 = (above_y(j, 2, i) - e2) - (e1z - e1)
            S[3, i] = roll(K[0, i] * c0, 1, 1)
            if i < NB - 1:
                S[4, i] = roll(K[1, i] * ((e0z - e0) - (field(j, 2, i + 1) - e2)), 1, 1)
            S[5, i] = roll(M[2, i] * (e2 + (phz - ph)), 1, 1)
            for n in range(3):
                T[n, i] = (scale * THETA) * v[n] + back * V[before, n, i]
            T[3, i] = (scale * THETA) * ph + back * field(before, 3, i)
            uv = uv + fold(v[0] * e0 + v[1] * e1 + v[2] * e2 + DN[i] * ph * ph)
        MOM[pl.ds(2 * j, 1), :] = jnp.sum(uv, axis=0, keepdims=True)

    def halo(slabs, i):
        return [roll(t, 126 - 2 * i, 1) for t in slabs]

    def fluxes_low(j, diag):
        e0, e1, e2, ph = (field(j, f, -1) for f in range(4))
        n1, n2, nph = (field(j, f, 0) for f in (1, 2, 3))
        e0z = last_lane(from_lanes(DR[j, 2], 127) if diag else 0.0, roll(e0, -1, 1))
        e0y = jnp.where(row_id() == 31, DR[j, 0, 0:1, :] if diag else 0.0, roll(e0, -1, 0))
        g1 = CX[0] * ((e0z - e0) - (n2 - e2))
        g2 = CX[1] * ((n1 - e1) - (e0y - e0))
        return g1, g2, CX[2] * (e0 + (nph - ph))

    def fluxes(j, i, ends):
        e0, e1, e2, ph = (field(j, f, i) for f in range(4))
        n1, n2, nph = (field(j, f, i + 1) for f in (1, 2, 3))
        e0z = last_lane(ends[0], S[0, i])
        e1z = last_lane(ends[1], S[1, i])
        phz = last_lane(ends[2], S[2, i])
        c0 = (above_y(j, 2, i) - e2) - (e1z - e1)
        c1 = (e0z - e0) - (n2 - e2)
        c2 = (n1 - e1) - (above_y(j, 0, i) - e0)
        u0 = e0 + (nph - ph)
        u1 = e1 + (above_y(j, 3, i) - ph)
        u2 = e2 + (phz - ph)
        return (c0, c1, c2), (u0, u1, u2)

    def operator(i, g, f, lo, ends):
        g0, g1, g2 = g
        f0, f1, f2 = f
        g1_lo, g2_lo, f0_lo = lo
        g0y = below_y(g0, LOW[0, i : i + 1, :])
        g2y = below_y(g2, LOW[1, i : i + 1, :])
        g0z = jnp.concatenate([S[3, i, 0:24], roll(g0[24:32], 1, 1)], axis=0)
        g0z = first_lane(ends[1], g0z)
        g1z = first_lane(ends[0], roll(g1, 1, 1) if i == NB - 1 else S[4, i])
        w0 = (g1z - g1) - (g2y - g2) + f0
        w1 = (g2_lo - g2) - (g0z - g0) + f1
        w2 = (g0y - g0) - (g1_lo - g1) + f2
        return w0, w1, w2

    def divergence(i, f, lo, ends):
        f1y = below_y(f[1], LOW[2, i : i + 1, :])
        f2z = first_lane(ends[2], S[5, i])
        return IDN[i] * ((lo[2] - f[0]) + (f1y - f[1]) + (f2z - f[2]))

    def one_round(j, carry):
        receive(j, (6, 7, 8, 9, 10, 11))
        scale = jnp.where(j == 0, F32(1.0 / SIGMA), F32(2.0 / SIGMA))
        rows_above(j)
        slabs = edges(j, False)

        def products(i):
            ends = halo(slabs, i)
            c, u = fluxes(j, i, ends)
            for n in range(3):
                U[j, n, i] = u[n]
            return [K[n, i] * c[n] for n in range(3)], [M[n, i] * u[n] for n in range(3)], ends

        def advance(i, slab, g, f, ends, lo):
            w = operator(i, g, f, lo, ends)
            q = divergence(i, f, lo, ends)
            w = [scale * w[n] - T[n, i] for n in range(3)]
            for n in range(3):
                V[j + 1, n, i] = w[n]
            s = {n: w[n] * ID[n, i] for n in range(3)}
            s[3] = scale * q - T[3, i]
            if i == 0:
                del s[1], s[2]
            if i == NB - 1:
                del s[0]
            return finish(j + 1, i, slab, s)

        slab = jnp.zeros((ROWS, LANES), F32)
        g, f, ends = products(0)
        plane_0 = (g, f, ends)
        for i in range(1, NB):
            lo = (g[1], g[2], f[0])
            if i == NB - 1:
                receive(j, (4, 5))
            g, f, ends = products(i)
            slab = advance(i, slab, g, f, ends, lo)
        slab = advance(0, slab, *plane_0, fluxes_low(j, False))
        receive(j, (0, 1, 2, 3))
        end = NB - 1
        xz = jnp.where(lane_id() == 0, CZ7[...] * from_lanes(DR[j, 3], 0), 0.0)
        xy = jnp.where(row_id() == 0, CY[1, end : end + 1, :] * DR[j, 1, 0:1, :], 0.0)
        w0 = V[j + 1, 0, end] - scale * (xy + xz)
        xy = jnp.where(row_id() == 31, CX[1, 31:32, :] * DR[j, 0, 0:1, :], 0.0)
        w1 = V[j + 1, 1, 0] - scale * xy
        xz = jnp.where(lane_id() == 127, CX[0] * from_lanes(DR[j, 2], 127), 0.0)
        w2 = V[j + 1, 2, 0] - scale * xz
        s0, s1, s2 = w0 * ID[0, end], w1 * ID[1, 0], w2 * ID[2, 0]
        diagonals(j + 1, s0, s1, s2)
        send(j + 1, (0, 1, 2, 3))
        slab = finish(j + 1, end, slab, {0: s0})
        slab = finish(j + 1, 0, slab, {1: s1, 2: s2})
        send(j + 1, (4, 5))
        V[j + 1, 0, end], V[j + 1, 1, 0], V[j + 1, 2, 0] = w0, w1, w2
        ZS[j + 1] = slab
        send(j + 1, LATE)
        ahead(j + 1)
        wu = jnp.zeros((8, LANES), F32)
        for i in range(NB):
            w = [V[j + 1, n, i] for n in range(3)]
            wu = wu + fold(w[0] * U[j, 0, i] + w[1] * U[j, 1, i] + w[2] * U[j, 2, i])
        MOM[pl.ds(2 * j + 1, 1), :] = jnp.sum(wu, axis=0, keepdims=True)
        return carry

    last = ITERS - 1
    ahead(0)
    lax.fori_loop(0, last, one_round, 0)

    core = lax.rem(gz, 2)
    group_a = [
        (dx, 0, 0 if dc == 0 else 1 - 2 * core)
        for dx in range(nx)
        for dc in range(2)
        if (dx, dc) != (0, 0)
    ]
    pair = [(0, 0, 1 - 2 * core)]
    chips = [
        (dx, dy, dz)
        for dx in range(nx)
        for dy in range(ny)
        for dz in range(0, nz, 2)
        if (dx, dy, dz) != (0, 0, 0)
    ]
    chips.sort(key=lambda o: -sum(min(d, n - d) for d, n in zip((o[0], o[1], o[2] // 2), (nx, ny, nz // 2))))
    group_b = [(0, dy, dz) for dy in range(ny) for dz in range(0, nz, 2) if (dy, dz) != (0, 0)]

    def spread(n, group, base, into):
        copies = [
            remote(SUM.at[n], into.at[k], a_send.at[base + k], a_recv.at[base + k], offset)
            for k, offset in enumerate(group)
        ]
        for c in copies:
            c.start()
        return copies

    def gather(n, copies, group, base, into):
        for c in copies:
            c.wait_recv()
        return SUM[n] + jnp.sum(into[base : base + len(group)], axis=0)

    n_a, n_b = len(group_a), len(group_b)
    SUM[0] = lanes_of(MOM[...])
    copies_0 = spread(0, group_a, 0, RA)

    receive(last, (9, 11, 5))
    rows_above(last)
    high = ZR[last, 1]
    au = jnp.zeros((8, LANES), F32)
    for i in range(NB):
        ends = [roll(high, 127 - place(f, i) - 1, 1) for f in (0, 1, 3)]
        c, u = fluxes(last, i, ends)
        g = [K[n, i] * c[n] for n in range(3)]
        f = [M[n, i] * u[n] for n in range(3)]
        for n in range(3):
            U[last, n, i] = u[n]
            G[n, i], G[3 + n, i] = g[n], f[n]
        au = au + fold(
            (g[0] * c[0] + g[1] * c[1] + g[2] * c[2]) + (f[0] * u[0] + f[1] * u[1] + f[2] * u[2])
        )
    au = jnp.sum(jnp.sum(au, axis=0, keepdims=True), axis=1, keepdims=True)
    SUM[1] = jnp.broadcast_to(au, (1, LANES))
    copies_1 = spread(1, pair, n_a + n_b, RC)
    SUM[3] = gather(1, copies_1, pair, 0, RC)
    copies_3 = spread(3, chips, n_a + n_b + 1, RD)
    SUM[2] = gather(0, copies_0, group_a, 0, RA)
    copies_2 = spread(2, group_b, n_a, RB)
    receive(last, (0, 1, 2, 3, 6, 7, 8, 10, 4))
    slabs = edges(last, True)
    scale = 2.0 / SIGMA

    def last_planes(planes):
        for i in planes:
            if i == 0:
                lo = fluxes_low(last, True)
            else:
                lo = (G[1, i - 1], G[2, i - 1], G[3, i - 1])
            ends = halo(slabs[0:2], i)
            w = operator(i, [G[n, i] for n in range(3)], [G[3 + n, i] for n in range(3)], lo, ends)
            for n in range(3):
                V[last + 1, n, i] = scale * w[n] - T[n, i]

    last_planes(range(0, NB))
    total = gather(2, copies_2, group_b, 0, RB)
    moment = [
        jnp.broadcast_to(jnp.sum(jnp.where(lane_id(1) == m, total, 0.0), axis=1, keepdims=True), (1, LANES))
        for m in range(2 * ITERS - 1)
    ]
    nu = moment[0:2]
    for m in range(2, 2 * ITERS - 1):
        nu.append(2.0 * moment[m] - nu[m % 2])
    cx, cp, cr, ca, gamma, slack, weight = cheb_coefficients(nu)
    for c in range(3):
        for i in range(NB):
            u = [U[j, c, i] for j in range(ITERS)]
            v = [V[j, c, i] for j in range(ITERS + 1)]
            x_out[c, i] = sum(cx[j] * u[j] for j in range(1, last)) + cx[0] * u[0]
            p_out[c, i] = sum(cp[j] * u[j] for j in range(1, ITERS)) + cp[0] * u[0]
            r_out[c, i] = sum(cr[j] * v[j] for j in range(1, ITERS)) + cr[0] * v[0]
            a_out[c, i] = sum(ca[j] * v[j] for j in range(1, ITERS + 1)) + ca[0] * v[0]

    def sent(j, carry):
        for c in messages(j, range(12)):
            c.wait_send()
        return carry

    lax.fori_loop(0, ITERS, sent, 0)
    for c in coef + copies_0 + copies_1 + copies_2 + copies_3:
        c.wait_send()
    au = gather(3, copies_3, chips, 0, RD)
    top = scale * (au - THETA * moment[2 * last]) - moment[2 * last - 1]
    alpha_out[...] = gamma / (slack + weight * (2.0 * top - nu[1]))


def body(sizes, right_side, mass_coef, curl_coef):
    shape = right_side.shape
    nx, ny, nz = sizes
    n_a = 2 * nx - 1
    n_b = ny * nz // 2 - 1
    n_c = nx * ny * nz // 2 - 1
    vm = lambda *s: pltpu.VMEM(s, F32)
    dma = lambda *s: pltpu.SemaphoreType.DMA(s)
    x, p, r, a, alpha = pl.pallas_call(
        functools.partial(kernel, sizes),
        out_shape=(pltpu.VMEM(shape, F32),) * 4 + (pltpu.VMEM((1, LANES), F32),),
        in_specs=[pl.BlockSpec(memory_space=pl.ANY)] * 3,
        out_specs=[pl.BlockSpec(memory_space=pltpu.VMEM)] * 5,
        scratch_shapes=[
            vm(5, *shape),
            vm(*shape),
            vm(*shape),
            vm(*shape),
            vm(*shape[1:]),
            vm(4, 4, 10, 48, LANES),
            vm(4, *shape),
            vm(6, *shape[1:]),
            vm(6, *shape[1:]),
            vm(4, *shape[1:]),
            vm(4, ROWS, LANES),
            vm(4, ROWS, LANES),
            vm(4, 8, LANES),
            vm(4, 8, LANES),
            vm(ROWS, LANES),
            vm(ROWS, LANES),
            vm(3, ROWS, LANES),
            vm(ROWS, LANES),
            vm(4, 7, 8, LANES),
            vm(4, 7, 8, LANES),
            vm(4, ROWS, LANES),
            vm(4, 2, ROWS, LANES),
            vm(4, 4, 8, LANES),
            vm(4, 6, 8, LANES),
            vm(3, 8, LANES),
            vm(*shape[1:]),
            vm(8, LANES),
            vm(4, 1, LANES),
            vm(n_a, 1, LANES),
            vm(n_b, 1, LANES),
            vm(1, 1, LANES),
            vm(n_c, 1, LANES),
            dma(6),
            dma(3),
            dma(3),
            dma(4, 12),
            dma(4, 12),
            dma(n_a + n_b + 1 + n_c),
            dma(n_a + n_b + 1 + n_c),
        ],
        compiler_params=pltpu.CompilerParams(collective_id=0, has_side_effects=True),
    )(right_side, mass_coef, curl_coef)
    step = jnp.broadcast_to(alpha[0], shape)
    return x + step * p, r - step * a


def solution(mesh):
    sizes = (mesh.shape["gx"], mesh.shape["gy"], mesh.shape["gz"])
    spec = P(None, "gx", "gy", "gz")
    return jax.shard_map(
        functools.partial(body, sizes),
        mesh=mesh,
        in_specs=(spec,) * 3,
        out_specs=(spec,) * 2,
        check_vma=False,
    )
```

```python
import functools
import jax
import jax.numpy as jnp
from jax import lax
from jax.experimental import pallas as pl
from jax.experimental.pallas import tpu as pltpu
from jax.sharding import PartitionSpec as P

ITERS = 4
THETA = 1.25
SIGMA = 1.25
MESH = pl.DeviceIdType.MESH
F32 = jnp.float32
NB = 8
ROWS = 32
LANES = 128
BASE = 8

ROUND = (
    (1, -1, 0),
    (-1, 1, 0),
    (1, 0, -1),
    (-1, 0, 1),
    (1, 0, 0),
    (-1, 0, 0),
    (0, 1, -1),
    (0, -1, 1),
    (0, 1, 0),
    (0, -1, 0),
    (0, 0, 1),
    (0, 0, -1),
)
UP = (0, 2, 4)
DOWN = (1, 3, 5)
LATE = (6, 7, 8, 9, 10, 11)
FACES = ((1, 0, 0), (-1, 0, 0), (0, 1, 0), (0, -1, 0), (0, 0, 1), (0, 0, -1))
START = (7, 6, 5, 4, 3, 2, 1, 0)


def lane_id(rows=ROWS):
    return lax.broadcasted_iota(jnp.int32, (rows, LANES), 1)


def row_id(rows=ROWS):
    return lax.broadcasted_iota(jnp.int32, (rows, LANES), 0)


def roll(v, amount, axis):
    amount = amount % v.shape[axis]
    return v if amount == 0 else pltpu.roll(v, amount, axis)


def place(field, plane):
    return 16 * field + 2 * plane


def packed(acc, v, field, plane):
    at = place(field, plane)
    return jnp.where((lane_id() >> 1) == at // 2, roll(v, at - 127, 1), acc)


def below_y(v, row):
    return jnp.where(row_id() == 0, row, roll(v, 1, 0))


def first_lane(halo, v):
    return jnp.where(lane_id() == 0, halo, v)


def last_lane(halo, v):
    return jnp.where(lane_id() == 127, halo, v)


def lanes_of(parts):
    sums = jnp.sum(parts, axis=1, keepdims=True)
    return jnp.sum(jnp.where(lane_id(8) == row_id(8), sums, 0.0), axis=0, keepdims=True)


def to_lanes(v, lane):
    out = jnp.zeros((8, LANES), F32)
    for b in range(4):
        out = jnp.where(lane_id(8) == b, roll(v[8 * b : 8 * b + 8], b - lane, 1), out)
    return out


def from_lanes(v, lane):
    return jnp.concatenate([roll(v, lane - b, 1) for b in range(4)], axis=0)


def fold(v):
    return v[0:8] + v[8:16] + v[16:24] + v[24:32]


def cheb_coefficients(nu):
    zero = jnp.zeros_like(nu[0])
    top = 2 * ITERS - 1

    def gram(i, j):
        if i + j == top:
            return 0.5 * nu[abs(i - j)]
        return 0.5 * (nu[i + j] + nu[abs(i - j)])

    def applied(c):
        out = [zero] * (len(c) + 1)
        for i, a in enumerate(c):
            if i == 0:
                out[1] = out[1] + a
            else:
                out[i + 1] = out[i + 1] + 0.5 * a
                out[i - 1] = out[i - 1] + 0.5 * a
        out = [SIGMA * a for a in out]
        for i, a in enumerate(c):
            out[i] = out[i] + THETA * a
        return out

    def dot(c, d):
        total = zero
        for i, a in enumerate(c):
            for j, b in enumerate(d):
                total = total + a * b * gram(i, j)
        return total

    res = [zero + 1.0]
    direction = None
    iterate = [zero] * ITERS
    gamma_old = alpha_old = None
    for iteration in range(ITERS):
        gamma = dot(res, res)
        image = applied(res)
        delta = dot(image, res)
        if iteration == 0:
            alpha = gamma / delta
            direction = list(res)
        else:
            beta = gamma / gamma_old
            slack = delta - beta * gamma / alpha_old
            direction = [
                a + (beta * direction[i] if i < len(direction) else zero) for i, a in enumerate(res)
            ]
            if iteration == ITERS - 1:
                return iterate, direction, res, applied(direction), gamma, slack, 0.5 * image[-1] * res[-1]
            alpha = gamma / slack
        for i, a in enumerate(direction):
            iterate[i] = iterate[i] + alpha * a
        step = applied(direction)
        res = [(res[i] if i < len(res) else zero) - alpha * a for i, a in enumerate(step)]
        gamma_old, alpha_old = gamma, alpha


def kernel(
    sizes,
    r_hbm,
    m_hbm,
    k_hbm,
    x_out,
    p_out,
    r_out,
    a_out,
    alpha_out,
    V,
    M,
    K,
    ID,
    IDN,
    F,
    U,
    G,
    S,
    T,
    XS,
    CX,
    CYS,
    CY,
    CZS,
    CZ,
    CZR,
    CZ7,
    YS,
    YR,
    ZS,
    ZR,
    DS,
    DR,
    DX,
    DXR,
    LOW,
    DN,
    MOM,
    SUM,
    RA,
    RB,
    RC,
    RD,
    load_sem,
    c_send,
    c_recv,
    n_send,
    n_recv,
    a_send,
    a_recv,
):
    nx, ny, nz = sizes
    gx, gy, gz = lax.axis_index("gx"), lax.axis_index("gy"), lax.axis_index("gz")

    def device(dx, dy, dz):
        return {
            "gx": lax.rem(gx + dx + nx, nx),
            "gy": lax.rem(gy + dy + ny, ny),
            "gz": lax.rem(gz + dz + nz, nz),
        }

    def remote(src, dst, send, recv, offset):
        return pltpu.make_async_remote_copy(
            src_ref=src,
            dst_ref=dst,
            send_sem=send,
            recv_sem=recv,
            device_id=device(*offset),
            device_id_type=MESH,
        )

    loads = [
        pltpu.make_async_copy(k_hbm, K, load_sem.at[0]),
        pltpu.make_async_copy(m_hbm, M, load_sem.at[1]),
        pltpu.make_async_copy(r_hbm, V.at[0], load_sem.at[2]),
    ]
    first = [
        pltpu.make_async_copy(k_hbm.at[1:3, NB - 1], XS.at[0:2], load_sem.at[3]),
        pltpu.make_async_copy(m_hbm.at[0, NB - 1], XS.at[2], load_sem.at[4]),
        pltpu.make_async_copy(r_hbm.at[0, NB - 1], XS.at[3], load_sem.at[5]),
    ]
    for c in first:
        c.start()
    for c in loads:
        c.start()
    barrier = pltpu.get_barrier_semaphore()
    for o in FACES:
        pl.semaphore_signal(barrier, inc=1, device_id=device(*o), device_id_type=MESH)
    coef = [
        remote(XS, CX, c_send.at[0], c_recv.at[0], (1, 0, 0)),
        remote(CYS, CY, c_send.at[1], c_recv.at[1], (0, 1, 0)),
        remote(CZS, CZ, c_send.at[2], c_recv.at[2], (0, 0, 1)),
    ]
    for c in first:
        c.wait()
    pl.semaphore_wait(barrier, len(FACES))
    coef[0].start()
    for c in loads:
        c.wait()
    y_fields = (K.at[0], K.at[2], M.at[1], V.at[0, 1])
    z_fields = (K.at[0], K.at[1], M.at[2], V.at[0, 2])
    for f, ref in enumerate(y_fields):
        for i in range(NB):
            CYS[f, i : i + 1, :] = ref[i, 31:32, :]
    coef[1].start()
    slab = jnp.zeros((ROWS, LANES), F32)
    for f, ref in enumerate(z_fields):
        for i in range(NB):
            slab = packed(slab, ref[i], f, i)
    CZS[...] = slab
    coef[2].start()
    for i in range(NB):
        S[0, i] = roll(K[0, i], 1, 1)
        S[1, i] = roll(K[1, i], 1, 1)
        S[2, i] = roll(M[2, i], 1, 1)
        S[3, i] = roll(V[0, 2, i], 1, 1)
    coef[1].wait_recv()
    coef[2].wait_recv()

    def messages(j, which):
        pairs = (
            (DX.at[j, 0], DXR.at[j, 0]),
            (DX.at[j, 1], DXR.at[j, 1]),
            (DS.at[j, 2], DR.at[j, 2]),
            (DS.at[j, 3], DR.at[j, 3]),
            (F.at[j, 0:4, NB, BASE : BASE + ROWS], F.at[j, 0:4, 0, BASE : BASE + ROWS]),
            (F.at[j, 1:4, 1, BASE : BASE + ROWS], F.at[j, 1:4, NB + 1, BASE : BASE + ROWS]),
            (YS.at[j, 1], DR.at[j, 4]),
            (ZS.at[j, 0:8], DR.at[j, 5]),
            (YS.at[j, 0:4], YR.at[j, 0:4]),
            (YS.at[j, 4:7], YR.at[j, 4:7]),
            (ZS.at[j], ZR.at[j, 0]),
            (ZS.at[j], ZR.at[j, 1]),
        )
        return [
            remote(*pairs[k], n_send.at[j, k], n_recv.at[j, k], ROUND[k]) for k in which
        ]

    def send(j, which):
        for c in messages(j, which):
            c.start()

    def receive(j, which):
        for c in messages(j, which):
            c.wait_recv()

    def finish(j, i, slab, values):
        for f, v in values.items():
            F[j, f, 1 + i, BASE : BASE + ROWS, :] = v
            YS[j, f, i : i + 1, :] = v[31:32]
            if f != 1:
                YS[j, (4, 0, 5, 6)[f], i : i + 1, :] = v[0:1]
            slab = packed(slab, v, f, i)
        return slab

    def diagonals(j, s0, s1, s2):
        if s0 is not None:
            DX[j, 0] = s0[0:1]
            DS[j, 2] = to_lanes(s0, 0)
        if s1 is not None:
            DX[j, 1] = s1[31:32]
            DS[j, 3] = to_lanes(s2, 127)

    slab = jnp.zeros((ROWS, LANES), F32)
    cz = CZ[...]
    for f in range(3):
        CZR[f] = roll(cz, 2 - 16 * f, 1)
    CZ7[...] = roll(cz, -place(1, NB - 1), 1)
    for i in START:
        if i == 0:
            coef[0].wait_recv()
        k0, k1, k2 = K[0, i], K[1, i], K[2, i]
        m0, m1, m2 = M[0, i], M[1, i], M[2, i]
        r0, r1, r2 = V[0, 0, i], V[0, 1, i], V[0, 2, i]
        if i == 0:
            k1_lo, k2_lo, m0_lo, r0_lo = CX[0], CX[1], CX[2], CX[3]
        else:
            k1_lo, k2_lo, m0_lo, r0_lo = K[1, i - 1], K[2, i - 1], M[0, i - 1], V[0, 0, i - 1]
        k0y = below_y(k0, CY[0, i : i + 1, :])
        k2y = below_y(k2, CY[1, i : i + 1, :])
        m1y = below_y(m1, CY[2, i : i + 1, :])
        r1y = below_y(r1, CY[3, i : i + 1, :])
        k0z = first_lane(roll(cz, -place(0, i), 1), S[0, i])
        k1z = first_lane(roll(cz, -place(1, i), 1), S[1, i])
        m2z = first_lane(roll(cz, -place(2, i), 1), S[2, i])
        r2z = first_lane(roll(cz, -place(3, i), 1), S[3, i])
        id0 = 1.0 / (m0 + k1 + k1z + k2 + k2y)
        id1 = 1.0 / (m1 + k2 + k2_lo + k0 + k0z)
        id2 = 1.0 / (m2 + k0 + k0y + k1 + k1_lo)
        dn = m0 + m0_lo + m1 + m1y + m2 + m2z
        idn = 1.0 / dn
        phi = idn * ((r0_lo - r0) + (r1y - r1) + (r2z - r2))
        ID[0, i], ID[1, i], ID[2, i], IDN[i], DN[i] = id0, id1, id2, idn, dn
        s0, s1, s2 = r0 * id0, r1 * id1, r2 * id2
        slab = finish(0, i, slab, {0: s0, 1: s1, 2: s2, 3: phi})
        diagonals(0, s0 if i == 7 else None, s1 if i == 0 else None, s2)
        if i == 7:
            send(0, UP)
        if i == 0:
            send(0, DOWN)
    ZS[0] = slab
    send(0, LATE)
    MOM[7:8, :] = jnp.zeros((1, LANES), F32)

    def field(j, f, i):
        return F[j, f, 1 + i, BASE : BASE + ROWS, :]

    def above_y(j, f, i):
        return F[j, f, 1 + i, BASE + 1 : BASE + 1 + ROWS, :]

    def rows_above(j):
        for f, at in ((0, 4), (2, 5), (3, 6)):
            for i in range(NB):
                F[j, f, 1 + i, BASE + ROWS : BASE + ROWS + 1, :] = YR[j, at, i : i + 1, :]

    def edges(j, diag):
        sub, lane8 = row_id(8), lane_id(8)
        s0, s1, s2, ph = YR[j, 0], YR[j, 1], YR[j, 2], YR[j, 3]
        own0, own2, own_ph = YS[j, 4], YS[j, 5], YS[j, 6]
        s1x = jnp.where(sub == 7, DXR[j, 1] if diag else 0.0, roll(s1, -1, 0))
        s1z = jnp.where(lane8 == 127, roll(DR[j, 4], -1, 1), roll(s1, -1, 1))
        LOW[0] = CY[0] * ((own2 - s2) - (s1z - s1))
        LOW[1] = CY[1] * ((s1x - s1) - (own0 - s0))
        LOW[2] = CY[2] * (s1 + (own_ph - ph))
        lane, row = lane_id(), row_id()
        low = jnp.where((lane & 1) == 1, ZS[j], ZR[j, 0])
        z0, z1, z2, zp = (roll(low, 2 - 16 * f, 1) for f in range(4))
        z2y = jnp.where(row == 31, roll(DR[j, 5], 2 - 32, 1)[0:1], roll(z2, -1, 0))
        z2x = jnp.where(lane == 16, from_lanes(DR[j, 3], 16) if diag else 0.0, roll(z2, -2, 1))
        gz0 = CZR[0] * ((z2y - z2) - (roll(z1, -1, 1) - z1))
        gz1 = CZR[1] * ((roll(z0, -1, 1) - z0) - (z2x - z2))
        mz2 = CZR[2] * (z2 + (roll(zp, -1, 1) - zp))
        odd = (lane & 1) == 1
        high = ZR[j, 1]
        return (
            jnp.where(odd, high, gz1),
            jnp.where(odd, roll(high, -16, 1), gz0),
            jnp.where(odd, roll(high, -48, 1), mz2),
        )

    def ahead(j):
        first = j == 0
        scale = jnp.where(first, F32(1.0 / SIGMA), F32(2.0 / SIGMA))
        back = jnp.where(first, F32(0.0), F32(1.0))
        before = jnp.maximum(j - 1, 0)
        uv = jnp.zeros((8, LANES), F32)
        for i in range(NB):
            e0, e1, e2, ph = (field(j, f, i) for f in range(4))
            v = [V[j, n, i] for n in range(3)]
            e0z, e1z, phz = roll(e0, -1, 1), roll(e1, -1, 1), roll(ph, -1, 1)
            S[0, i], S[1, i], S[2, i] = e0z, e1z, phz
            c0 = (above_y(j, 2, i) - e2) - (e1z - e1)
            S[3, i] = roll(K[0, i] * c0, 1, 1)
            if i < NB - 1:
                S[4, i] = roll(K[1, i] * ((e0z - e0) - (field(j, 2, i + 1) - e2)), 1, 1)
            S[5, i] = roll(M[2, i] * (e2 + (phz - ph)), 1, 1)
            for n in range(3):
                T[n, i] = (scale * THETA) * v[n] + back * V[before, n, i]
            T[3, i] = (scale * THETA) * ph + back * field(before, 3, i)
            uv = uv + fold(v[0] * e0 + v[1] * e1 + v[2] * e2 + DN[i] * ph * ph)
        MOM[pl.ds(2 * j, 1), :] = jnp.sum(uv, axis=0, keepdims=True)

    def halo(slabs, i):
        return [roll(t, 126 - 2 * i, 1) for t in slabs]

    def fluxes_low(j, diag):
        e0, e1, e2, ph = (field(j, f, -1) for f in range(4))
        n1, n2, nph = (field(j, f, 0) for f in (1, 2, 3))
        e0z = last_lane(from_lanes(DR[j, 2], 127) if diag else 0.0, roll(e0, -1, 1))
        e0y = jnp.where(row_id() == 31, DXR[j, 0] if diag else 0.0, roll(e0, -1, 0))
        g1 = CX[0] * ((e0z - e0) - (n2 - e2))
        g2 = CX[1] * ((n1 - e1) - (e0y - e0))
        return g1, g2, CX[2] * (e0 + (nph - ph))

    def fluxes(j, i, ends):
        e0, e1, e2, ph = (field(j, f, i) for f in range(4))
        n1, n2, nph = (field(j, f, i + 1) for f in (1, 2, 3))
        e0z = last_lane(ends[0], S[0, i])
        e1z = last_lane(ends[1], S[1, i])
        phz = last_lane(ends[2], S[2, i])
        c0 = (above_y(j, 2, i) - e2) - (e1z - e1)
        c1 = (e0z - e0) - (n2 - e2)
        c2 = (n1 - e1) - (above_y(j, 0, i) - e0)
        u0 = e0 + (nph - ph)
        u1 = e1 + (above_y(j, 3, i) - ph)
        u2 = e2 + (phz - ph)
        return (c0, c1, c2), (u0, u1, u2)

    def operator(i, g, f, lo, ends):
        g0, g1, g2 = g
        f0, f1, f2 = f
        g1_lo, g2_lo, f0_lo = lo
        g0y = below_y(g0, LOW[0, i : i + 1, :])
        g2y = below_y(g2, LOW[1, i : i + 1, :])
        g0z = jnp.concatenate([S[3, i, 0:24], roll(g0[24:32], 1, 1)], axis=0)
        g0z = first_lane(ends[1], g0z)
        g1z = first_lane(ends[0], roll(g1, 1, 1) if i == NB - 1 else S[4, i])
        w0 = (g1z - g1) - (g2y - g2) + f0
        w1 = (g2_lo - g2) - (g0z - g0) + f1
        w2 = (g0y - g0) - (g1_lo - g1) + f2
        return w0, w1, w2

    def divergence(i, f, lo, ends):
        f1y = below_y(f[1], LOW[2, i : i + 1, :])
        f2z = first_lane(ends[2], S[5, i])
        return IDN[i] * ((lo[2] - f[0]) + (f1y - f[1]) + (f2z - f[2]))

    def one_round(j, carry):
        receive(j, (6, 7, 8, 9, 10, 11))
        scale = jnp.where(j == 0, F32(1.0 / SIGMA), F32(2.0 / SIGMA))
        rows_above(j)
        slabs = edges(j, False)

        def products(i):
            ends = halo(slabs, i)
            c, u = fluxes(j, i, ends)
            for n in range(3):
                U[j, n, i] = u[n]
            return [K[n, i] * c[n] for n in range(3)], [M[n, i] * u[n] for n in range(3)], ends

        def advance(i, slab, g, f, ends, lo):
            w = operator(i, g, f, lo, ends)
            q = divergence(i, f, lo, ends)
            w = [scale * w[n] - T[n, i] for n in range(3)]
            for n in range(3):
                V[j + 1, n, i] = w[n]
            s = {n: w[n] * ID[n, i] for n in range(3)}
            s[3] = scale * q - T[3, i]
            if i == 0:
                del s[1], s[2]
            if i == NB - 1:
                del s[0]
            return finish(j + 1, i, slab, s)

        slab = jnp.zeros((ROWS, LANES), F32)
        g, f, ends = products(0)
        plane_0 = (g, f, ends)
        for i in range(1, NB):
            lo = (g[1], g[2], f[0])
            if i == NB - 1:
                receive(j, (4, 5))
            g, f, ends = products(i)
            slab = advance(i, slab, g, f, ends, lo)
        slab = advance(0, slab, *plane_0, fluxes_low(j, False))
        receive(j, (0, 1, 2, 3))
        end = NB - 1
        xz = jnp.where(lane_id() == 0, CZ7[...] * from_lanes(DR[j, 3], 0), 0.0)
        xy = jnp.where(row_id() == 0, CY[1, end : end + 1, :] * DXR[j, 1], 0.0)
        w0 = V[j + 1, 0, end] - scale * (xy + xz)
        xy = jnp.where(row_id() == 31, CX[1, 31:32, :] * DXR[j, 0], 0.0)
        w1 = V[j + 1, 1, 0] - scale * xy
        xz = jnp.where(lane_id() == 127, CX[0] * from_lanes(DR[j, 2], 127), 0.0)
        w2 = V[j + 1, 2, 0] - scale * xz
        s0, s1, s2 = w0 * ID[0, end], w1 * ID[1, 0], w2 * ID[2, 0]
        diagonals(j + 1, s0, s1, s2)
        send(j + 1, (0, 1, 2, 3))
        slab = finish(j + 1, end, slab, {0: s0})
        slab = finish(j + 1, 0, slab, {1: s1, 2: s2})
        send(j + 1, (4, 5))
        V[j + 1, 0, end], V[j + 1, 1, 0], V[j + 1, 2, 0] = w0, w1, w2
        ZS[j + 1] = slab
        send(j + 1, LATE)
        ahead(j + 1)
        wu = jnp.zeros((8, LANES), F32)
        for i in range(NB):
            w = [V[j + 1, n, i] for n in range(3)]
            wu = wu + fold(w[0] * U[j, 0, i] + w[1] * U[j, 1, i] + w[2] * U[j, 2, i])
        MOM[pl.ds(2 * j + 1, 1), :] = jnp.sum(wu, axis=0, keepdims=True)
        return carry

    last = ITERS - 1
    ahead(0)
    lax.fori_loop(0, last, one_round, 0)

    core = lax.rem(gz, 2)
    group_a = [
        (dx, 0, 0 if dc == 0 else 1 - 2 * core)
        for dx in range(nx)
        for dc in range(2)
        if (dx, dc) != (0, 0)
    ]
    pair = [(0, 0, 1 - 2 * core)]
    chips = [
        (dx, dy, dz)
        for dx in range(nx)
        for dy in range(ny)
        for dz in range(0, nz, 2)
        if (dx, dy, dz) != (0, 0, 0)
    ]
    chips.sort(key=lambda o: -sum(min(d, n - d) for d, n in zip((o[0], o[1], o[2] // 2), (nx, ny, nz // 2))))
    group_b = [(0, dy, dz) for dy in range(ny) for dz in range(0, nz, 2) if (dy, dz) != (0, 0)]

    def spread(n, group, base, into):
        copies = [
            remote(SUM.at[n], into.at[k], a_send.at[base + k], a_recv.at[base + k], offset)
            for k, offset in enumerate(group)
        ]
        for c in copies:
            c.start()
        return copies

    def gather(n, copies, group, base, into):
        for c in copies:
            c.wait_recv()
        return SUM[n] + jnp.sum(into[base : base + len(group)], axis=0)

    n_a, n_b = len(group_a), len(group_b)
    SUM[0] = lanes_of(MOM[...])
    copies_0 = spread(0, group_a, 0, RA)

    receive(last, (9, 11))
    rows_above(last)
    high = ZR[last, 1]
    au = jnp.zeros((8, LANES), F32)
    for i in range(NB):
        if i == NB - 1:
            receive(last, (5,))
        ends = [roll(high, 127 - place(f, i) - 1, 1) for f in (0, 1, 3)]
        c, u = fluxes(last, i, ends)
        g = [K[n, i] * c[n] for n in range(3)]
        f = [M[n, i] * u[n] for n in range(3)]
        for n in range(3):
            U[last, n, i] = u[n]
            G[n, i], G[3 + n, i] = g[n], f[n]
        au = au + fold(
            (g[0] * c[0] + g[1] * c[1] + g[2] * c[2]) + (f[0] * u[0] + f[1] * u[1] + f[2] * u[2])
        )
    au = jnp.sum(jnp.sum(au, axis=0, keepdims=True), axis=1, keepdims=True)
    SUM[1] = jnp.broadcast_to(au, (1, LANES))
    copies_1 = spread(1, pair, n_a + n_b, RC)
    SUM[3] = gather(1, copies_1, pair, 0, RC)
    copies_3 = spread(3, chips, n_a + n_b + 1, RD)
    SUM[2] = gather(0, copies_0, group_a, 0, RA)
    copies_2 = spread(2, group_b, n_a, RB)
    receive(last, (0, 1, 2, 3, 6, 7, 8, 10, 4))
    slabs = edges(last, True)
    scale = 2.0 / SIGMA

    def last_planes(planes):
        for i in planes:
            if i == 0:
                lo = fluxes_low(last, True)
            else:
                lo = (G[1, i - 1], G[2, i - 1], G[3, i - 1])
            ends = halo(slabs[0:2], i)
            w = operator(i, [G[n, i] for n in range(3)], [G[3 + n, i] for n in range(3)], lo, ends)
            for n in range(3):
                V[last + 1, n, i] = scale * w[n] - T[n, i]

    last_planes(range(0, NB))
    total = gather(2, copies_2, group_b, 0, RB)
    moment = [
        jnp.broadcast_to(jnp.sum(jnp.where(lane_id(1) == m, total, 0.0), axis=1, keepdims=True), (1, LANES))
        for m in range(2 * ITERS - 1)
    ]
    nu = moment[0:2]
    for m in range(2, 2 * ITERS - 1):
        nu.append(2.0 * moment[m] - nu[m % 2])
    cx, cp, cr, ca, gamma, slack, weight = cheb_coefficients(nu)
    for c in range(3):
        for i in range(NB):
            u = [U[j, c, i] for j in range(ITERS)]
            v = [V[j, c, i] for j in range(ITERS + 1)]
            x_out[c, i] = sum(cx[j] * u[j] for j in range(1, last)) + cx[0] * u[0]
            p_out[c, i] = sum(cp[j] * u[j] for j in range(1, ITERS)) + cp[0] * u[0]
            r_out[c, i] = sum(cr[j] * v[j] for j in range(1, ITERS)) + cr[0] * v[0]
            a_out[c, i] = sum(ca[j] * v[j] for j in range(1, ITERS + 1)) + ca[0] * v[0]

    def sent(j, carry):
        for c in messages(j, range(12)):
            c.wait_send()
        return carry

    lax.fori_loop(0, ITERS, sent, 0)
    for c in coef + copies_0 + copies_1 + copies_2 + copies_3:
        c.wait_send()
    au = gather(3, copies_3, chips, 0, RD)
    top = scale * (au - THETA * moment[2 * last]) - moment[2 * last - 1]
    alpha_out[...] = gamma / (slack + weight * (2.0 * top - nu[1]))


def body(sizes, right_side, mass_coef, curl_coef):
    shape = right_side.shape
    nx, ny, nz = sizes
    n_a = 2 * nx - 1
    n_b = ny * nz // 2 - 1
    n_c = nx * ny * nz // 2 - 1
    vm = lambda *s: pltpu.VMEM(s, F32)
    dma = lambda *s: pltpu.SemaphoreType.DMA(s)
    x, p, r, a, alpha = pl.pallas_call(
        functools.partial(kernel, sizes),
        out_shape=(pltpu.VMEM(shape, F32),) * 4 + (pltpu.VMEM((1, LANES), F32),),
        in_specs=[pl.BlockSpec(memory_space=pl.ANY)] * 3,
        out_specs=[pl.BlockSpec(memory_space=pltpu.VMEM)] * 5,
        scratch_shapes=[
            vm(5, *shape),
            vm(*shape),
            vm(*shape),
            vm(*shape),
            vm(*shape[1:]),
            vm(4, 4, 10, 48, LANES),
            vm(4, *shape),
            vm(6, *shape[1:]),
            vm(6, *shape[1:]),
            vm(4, *shape[1:]),
            vm(4, ROWS, LANES),
            vm(4, ROWS, LANES),
            vm(4, 8, LANES),
            vm(4, 8, LANES),
            vm(ROWS, LANES),
            vm(ROWS, LANES),
            vm(3, ROWS, LANES),
            vm(ROWS, LANES),
            vm(4, 7, 8, LANES),
            vm(4, 7, 8, LANES),
            vm(4, ROWS, LANES),
            vm(4, 2, ROWS, LANES),
            vm(4, 4, 8, LANES),
            vm(4, 6, 8, LANES),
            vm(4, 2, 1, LANES),
            vm(4, 2, 1, LANES),
            vm(3, 8, LANES),
            vm(*shape[1:]),
            vm(8, LANES),
            vm(4, 1, LANES),
            vm(n_a, 1, LANES),
            vm(n_b, 1, LANES),
            vm(1, 1, LANES),
            vm(n_c, 1, LANES),
            dma(6),
            dma(3),
            dma(3),
            dma(4, 12),
            dma(4, 12),
            dma(n_a + n_b + 1 + n_c),
            dma(n_a + n_b + 1 + n_c),
        ],
        compiler_params=pltpu.CompilerParams(collective_id=0, has_side_effects=True),
    )(right_side, mass_coef, curl_coef)
    step = jnp.broadcast_to(alpha[0], shape)
    return x + step * p, r - step * a


def solution(mesh):
    sizes = (mesh.shape["gx"], mesh.shape["gy"], mesh.shape["gz"])
    spec = P(None, "gx", "gy", "gz")
    return jax.shard_map(
        functools.partial(body, sizes),
        mesh=mesh,
        in_specs=(spec,) * 3,
        out_specs=(spec,) * 2,
        check_vma=False,
    )
```

```python
import functools
import jax
import jax.numpy as jnp
from jax import lax
from jax.experimental import pallas as pl
from jax.experimental.pallas import tpu as pltpu
from jax.sharding import PartitionSpec as P

ITERS = 4
THETA = 1.25
SIGMA = 1.25
MESH = pl.DeviceIdType.MESH
F32 = jnp.float32
NB = 8
ROWS = 32
LANES = 128
BASE = 8

ROUND = (
    (1, -1, 0),
    (-1, 1, 0),
    (1, 0, -1),
    (-1, 0, 1),
    (1, 0, 0),
    (-1, 0, 0),
    (0, 1, -1),
    (0, -1, 1),
    (0, 1, 0),
    (0, -1, 0),
    (0, 0, 1),
    (0, 0, -1),
)
UP = (0, 2, 4)
DOWN = (1, 3, 5)
LATE = (6, 7, 9, 11, 8, 10)
FACES = ((1, 0, 0), (-1, 0, 0), (0, 1, 0), (0, -1, 0), (0, 0, 1), (0, 0, -1))
START = (7, 6, 5, 4, 3, 2, 1, 0)


def lane_id(rows=ROWS):
    return lax.broadcasted_iota(jnp.int32, (rows, LANES), 1)


def row_id(rows=ROWS):
    return lax.broadcasted_iota(jnp.int32, (rows, LANES), 0)


def roll(v, amount, axis):
    amount = amount % v.shape[axis]
    return v if amount == 0 else pltpu.roll(v, amount, axis)


def place(field, plane):
    return 16 * field + 2 * plane


def packed(acc, v, field, plane):
    at = place(field, plane)
    return jnp.where((lane_id() >> 1) == at // 2, roll(v, at - 127, 1), acc)


def below_y(v, row):
    return jnp.where(row_id() == 0, row, roll(v, 1, 0))


def first_lane(halo, v):
    return jnp.where(lane_id() == 0, halo, v)


def last_lane(halo, v):
    return jnp.where(lane_id() == 127, halo, v)


def lanes_of(parts):
    sums = jnp.sum(parts, axis=1, keepdims=True)
    return jnp.sum(jnp.where(lane_id(8) == row_id(8), sums, 0.0), axis=0, keepdims=True)


def to_lanes(v, lane):
    out = jnp.zeros((8, LANES), F32)
    for b in range(4):
        out = jnp.where(lane_id(8) == b, roll(v[8 * b : 8 * b + 8], b - lane, 1), out)
    return out


def from_lanes(v, lane):
    return jnp.concatenate([roll(v, lane - b, 1) for b in range(4)], axis=0)


def fold(v):
    return v[0:8] + v[8:16] + v[16:24] + v[24:32]


def cheb_coefficients(nu):
    zero = jnp.zeros_like(nu[0])
    top = 2 * ITERS - 1

    def gram(i, j):
        if i + j == top:
            return 0.5 * nu[abs(i - j)]
        return 0.5 * (nu[i + j] + nu[abs(i - j)])

    def applied(c):
        out = [zero] * (len(c) + 1)
        for i, a in enumerate(c):
            if i == 0:
                out[1] = out[1] + a
            else:
                out[i + 1] = out[i + 1] + 0.5 * a
                out[i - 1] = out[i - 1] + 0.5 * a
        out = [SIGMA * a for a in out]
        for i, a in enumerate(c):
            out[i] = out[i] + THETA * a
        return out

    def dot(c, d):
        total = zero
        for i, a in enumerate(c):
            for j, b in enumerate(d):
                total = total + a * b * gram(i, j)
        return total

    res = [zero + 1.0]
    direction = None
    iterate = [zero] * ITERS
    gamma_old = alpha_old = None
    for iteration in range(ITERS):
        gamma = dot(res, res)
        image = applied(res)
        delta = dot(image, res)
        if iteration == 0:
            alpha = gamma / delta
            direction = list(res)
        else:
            beta = gamma / gamma_old
            slack = delta - beta * gamma / alpha_old
            direction = [
                a + (beta * direction[i] if i < len(direction) else zero) for i, a in enumerate(res)
            ]
            if iteration == ITERS - 1:
                return iterate, direction, res, applied(direction), gamma, slack, 0.5 * image[-1] * res[-1]
            alpha = gamma / slack
        for i, a in enumerate(direction):
            iterate[i] = iterate[i] + alpha * a
        step = applied(direction)
        res = [(res[i] if i < len(res) else zero) - alpha * a for i, a in enumerate(step)]
        gamma_old, alpha_old = gamma, alpha


def kernel(
    sizes,
    r_hbm,
    m_hbm,
    k_hbm,
    x_out,
    p_out,
    r_out,
    a_out,
    alpha_out,
    V,
    M,
    K,
    ID,
    IDN,
    F,
    U,
    G,
    S,
    T,
    XS,
    CX,
    CYS,
    CY,
    CZS,
    CZ,
    CZR,
    CZ7,
    YS,
    YR,
    ZS,
    ZR,
    DS,
    DR,
    DX,
    DXR,
    LOW,
    DN,
    MOM,
    SUM,
    RA,
    RB,
    RC,
    RD,
    load_sem,
    c_send,
    c_recv,
    n_send,
    n_recv,
    a_send,
    a_recv,
):
    nx, ny, nz = sizes
    gx, gy, gz = lax.axis_index("gx"), lax.axis_index("gy"), lax.axis_index("gz")

    def device(dx, dy, dz):
        return {
            "gx": lax.rem(gx + dx + nx, nx),
            "gy": lax.rem(gy + dy + ny, ny),
            "gz": lax.rem(gz + dz + nz, nz),
        }

    def remote(src, dst, send, recv, offset):
        return pltpu.make_async_remote_copy(
            src_ref=src,
            dst_ref=dst,
            send_sem=send,
            recv_sem=recv,
            device_id=device(*offset),
            device_id_type=MESH,
        )

    loads = [
        pltpu.make_async_copy(k_hbm, K, load_sem.at[0]),
        pltpu.make_async_copy(m_hbm, M, load_sem.at[1]),
        pltpu.make_async_copy(r_hbm, V.at[0], load_sem.at[2]),
    ]
    first = [
        pltpu.make_async_copy(k_hbm.at[1:3, NB - 1], XS.at[0:2], load_sem.at[3]),
        pltpu.make_async_copy(m_hbm.at[0, NB - 1], XS.at[2], load_sem.at[4]),
        pltpu.make_async_copy(r_hbm.at[0, NB - 1], XS.at[3], load_sem.at[5]),
    ]
    for c in first:
        c.start()
    for c in loads:
        c.start()
    barrier = pltpu.get_barrier_semaphore()
    for o in FACES:
        pl.semaphore_signal(barrier, inc=1, device_id=device(*o), device_id_type=MESH)
    coef = [
        remote(XS, CX, c_send.at[0], c_recv.at[0], (1, 0, 0)),
        remote(CYS, CY, c_send.at[1], c_recv.at[1], (0, 1, 0)),
        remote(CZS, CZ, c_send.at[2], c_recv.at[2], (0, 0, 1)),
    ]
    for c in first:
        c.wait()
    pl.semaphore_wait(barrier, len(FACES))
    coef[0].start()
    for c in loads:
        c.wait()
    y_fields = (K.at[0], K.at[2], M.at[1], V.at[0, 1])
    z_fields = (K.at[0], K.at[1], M.at[2], V.at[0, 2])
    for f, ref in enumerate(y_fields):
        for i in range(NB):
            CYS[f, i : i + 1, :] = ref[i, 31:32, :]
    coef[1].start()
    slab = jnp.zeros((ROWS, LANES), F32)
    for f, ref in enumerate(z_fields):
        for i in range(NB):
            slab = packed(slab, ref[i], f, i)
    CZS[...] = slab
    coef[2].start()
    for i in range(NB):
        S[0, i] = roll(K[0, i], 1, 1)
        S[1, i] = roll(K[1, i], 1, 1)
        S[2, i] = roll(M[2, i], 1, 1)
        S[3, i] = roll(V[0, 2, i], 1, 1)
    coef[1].wait_recv()
    coef[2].wait_recv()

    def messages(j, which):
        pairs = (
            (DX.at[j, 0], DXR.at[j, 0]),
            (DX.at[j, 1], DXR.at[j, 1]),
            (DS.at[j, 2], DR.at[j, 2]),
            (DS.at[j, 3], DR.at[j, 3]),
            (F.at[j, 0:4, NB, BASE : BASE + ROWS], F.at[j, 0:4, 0, BASE : BASE + ROWS]),
            (F.at[j, 1:4, 1, BASE : BASE + ROWS], F.at[j, 1:4, NB + 1, BASE : BASE + ROWS]),
            (YS.at[j, 1], DR.at[j, 4]),
            (ZS.at[j, 0:8], DR.at[j, 5]),
            (YS.at[j, 0:4], YR.at[j, 0:4]),
            (YS.at[j, 4:7], YR.at[j, 4:7]),
            (ZS.at[j], ZR.at[j, 0]),
            (ZS.at[j], ZR.at[j, 1]),
        )
        return [
            remote(*pairs[k], n_send.at[j, k], n_recv.at[j, k], ROUND[k]) for k in which
        ]

    def send(j, which):
        for c in messages(j, which):
            c.start()

    def receive(j, which):
        for c in messages(j, which):
            c.wait_recv()

    def finish(j, i, slab, values):
        for f, v in values.items():
            F[j, f, 1 + i, BASE : BASE + ROWS, :] = v
            YS[j, f, i : i + 1, :] = v[31:32]
            if f != 1:
                YS[j, (4, 0, 5, 6)[f], i : i + 1, :] = v[0:1]
            slab = packed(slab, v, f, i)
        return slab

    def diagonals(j, s0, s1, s2):
        if s0 is not None:
            DX[j, 0] = s0[0:1]
            DS[j, 2] = to_lanes(s0, 0)
        if s1 is not None:
            DX[j, 1] = s1[31:32]
            DS[j, 3] = to_lanes(s2, 127)

    slab = jnp.zeros((ROWS, LANES), F32)
    cz = CZ[...]
    for f in range(3):
        CZR[f] = roll(cz, 2 - 16 * f, 1)
    CZ7[...] = roll(cz, -place(1, NB - 1), 1)
    for i in START:
        if i == 0:
            coef[0].wait_recv()
        k0, k1, k2 = K[0, i], K[1, i], K[2, i]
        m0, m1, m2 = M[0, i], M[1, i], M[2, i]
        r0, r1, r2 = V[0, 0, i], V[0, 1, i], V[0, 2, i]
        if i == 0:
            k1_lo, k2_lo, m0_lo, r0_lo = CX[0], CX[1], CX[2], CX[3]
        else:
            k1_lo, k2_lo, m0_lo, r0_lo = K[1, i - 1], K[2, i - 1], M[0, i - 1], V[0, 0, i - 1]
        k0y = below_y(k0, CY[0, i : i + 1, :])
        k2y = below_y(k2, CY[1, i : i + 1, :])
        m1y = below_y(m1, CY[2, i : i + 1, :])
        r1y = below_y(r1, CY[3, i : i + 1, :])
        k0z = first_lane(roll(cz, -place(0, i), 1), S[0, i])
        k1z = first_lane(roll(cz, -place(1, i), 1), S[1, i])
        m2z = first_lane(roll(cz, -place(2, i), 1), S[2, i])
        r2z = first_lane(roll(cz, -place(3, i), 1), S[3, i])
        id0 = 1.0 / (m0 + k1 + k1z + k2 + k2y)
        id1 = 1.0 / (m1 + k2 + k2_lo + k0 + k0z)
        id2 = 1.0 / (m2 + k0 + k0y + k1 + k1_lo)
        dn = m0 + m0_lo + m1 + m1y + m2 + m2z
        idn = 1.0 / dn
        phi = idn * ((r0_lo - r0) + (r1y - r1) + (r2z - r2))
        ID[0, i], ID[1, i], ID[2, i], IDN[i], DN[i] = id0, id1, id2, idn, dn
        s0, s1, s2 = r0 * id0, r1 * id1, r2 * id2
        slab = finish(0, i, slab, {0: s0, 1: s1, 2: s2, 3: phi})
        diagonals(0, s0 if i == 7 else None, s1 if i == 0 else None, s2)
        if i == 7:
            send(0, UP)
        if i == 0:
            send(0, DOWN)
    ZS[0] = slab
    send(0, LATE)
    MOM[7:8, :] = jnp.zeros((1, LANES), F32)

    def field(j, f, i):
        return F[j, f, 1 + i, BASE : BASE + ROWS, :]

    def above_y(j, f, i):
        return F[j, f, 1 + i, BASE + 1 : BASE + 1 + ROWS, :]

    def rows_above(j):
        for f, at in ((0, 4), (2, 5), (3, 6)):
            for i in range(NB):
                F[j, f, 1 + i, BASE + ROWS : BASE + ROWS + 1, :] = YR[j, at, i : i + 1, :]

    def edges(j, diag):
        sub, lane8 = row_id(8), lane_id(8)
        s0, s1, s2, ph = YR[j, 0], YR[j, 1], YR[j, 2], YR[j, 3]
        own0, own2, own_ph = YS[j, 4], YS[j, 5], YS[j, 6]
        s1x = jnp.where(sub == 7, DXR[j, 1] if diag else 0.0, roll(s1, -1, 0))
        s1z = jnp.where(lane8 == 127, roll(DR[j, 4], -1, 1), roll(s1, -1, 1))
        LOW[0] = CY[0] * ((own2 - s2) - (s1z - s1))
        LOW[1] = CY[1] * ((s1x - s1) - (own0 - s0))
        LOW[2] = CY[2] * (s1 + (own_ph - ph))
        lane, row = lane_id(), row_id()
        low = jnp.where((lane & 1) == 1, ZS[j], ZR[j, 0])
        z0, z1, z2, zp = (roll(low, 2 - 16 * f, 1) for f in range(4))
        z2y = jnp.where(row == 31, roll(DR[j, 5], 2 - 32, 1)[0:1], roll(z2, -1, 0))
        z2x = jnp.where(lane == 16, from_lanes(DR[j, 3], 16) if diag else 0.0, roll(z2, -2, 1))
        gz0 = CZR[0] * ((z2y - z2) - (roll(z1, -1, 1) - z1))
        gz1 = CZR[1] * ((roll(z0, -1, 1) - z0) - (z2x - z2))
        mz2 = CZR[2] * (z2 + (roll(zp, -1, 1) - zp))
        odd = (lane & 1) == 1
        high = ZR[j, 1]
        return (
            jnp.where(odd, high, gz1),
            jnp.where(odd, roll(high, -16, 1), gz0),
            jnp.where(odd, roll(high, -48, 1), mz2),
        )

    def ahead(j):
        first = j == 0
        scale = jnp.where(first, F32(1.0 / SIGMA), F32(2.0 / SIGMA))
        back = jnp.where(first, F32(0.0), F32(1.0))
        before = jnp.maximum(j - 1, 0)
        uv = jnp.zeros((8, LANES), F32)
        for i in range(NB):
            e0, e1, e2, ph = (field(j, f, i) for f in range(4))
            v = [V[j, n, i] for n in range(3)]
            e0z, e1z, phz = roll(e0, -1, 1), roll(e1, -1, 1), roll(ph, -1, 1)
            S[0, i], S[1, i], S[2, i] = e0z, e1z, phz
            c0 = (above_y(j, 2, i) - e2) - (e1z - e1)
            S[3, i] = roll(K[0, i] * c0, 1, 1)
            if i < NB - 1:
                S[4, i] = roll(K[1, i] * ((e0z - e0) - (field(j, 2, i + 1) - e2)), 1, 1)
            S[5, i] = roll(M[2, i] * (e2 + (phz - ph)), 1, 1)
            for n in range(3):
                T[n, i] = (scale * THETA) * v[n] + back * V[before, n, i]
            T[3, i] = (scale * THETA) * ph + back * field(before, 3, i)
            uv = uv + fold(v[0] * e0 + v[1] * e1 + v[2] * e2 + DN[i] * ph * ph)
        MOM[pl.ds(2 * j, 1), :] = jnp.sum(uv, axis=0, keepdims=True)

    def halo(slabs, i):
        return [roll(t, 126 - 2 * i, 1) for t in slabs]

    def fluxes_low(j, diag):
        e0, e1, e2, ph = (field(j, f, -1) for f in range(4))
        n1, n2, nph = (field(j, f, 0) for f in (1, 2, 3))
        e0z = last_lane(from_lanes(DR[j, 2], 127) if diag else 0.0, roll(e0, -1, 1))
        e0y = jnp.where(row_id() == 31, DXR[j, 0] if diag else 0.0, roll(e0, -1, 0))
        g1 = CX[0] * ((e0z - e0) - (n2 - e2))
        g2 = CX[1] * ((n1 - e1) - (e0y - e0))
        return g1, g2, CX[2] * (e0 + (nph - ph))

    def fluxes(j, i, ends):
        e0, e1, e2, ph = (field(j, f, i) for f in range(4))
        n1, n2, nph = (field(j, f, i + 1) for f in (1, 2, 3))
        e0z = last_lane(ends[0], S[0, i])
        e1z = last_lane(ends[1], S[1, i])
        phz = last_lane(ends[2], S[2, i])
        c0 = (above_y(j, 2, i) - e2) - (e1z - e1)
        c1 = (e0z - e0) - (n2 - e2)
        c2 = (n1 - e1) - (above_y(j, 0, i) - e0)
        u0 = e0 + (nph - ph)
        u1 = e1 + (above_y(j, 3, i) - ph)
        u2 = e2 + (phz - ph)
        return (c0, c1, c2), (u0, u1, u2)

    def operator(i, g, f, lo, ends):
        g0, g1, g2 = g
        f0, f1, f2 = f
        g1_lo, g2_lo, f0_lo = lo
        g0y = below_y(g0, LOW[0, i : i + 1, :])
        g2y = below_y(g2, LOW[1, i : i + 1, :])
        g0z = jnp.concatenate([S[3, i, 0:24], roll(g0[24:32], 1, 1)], axis=0)
        g0z = first_lane(ends[1], g0z)
        g1z = first_lane(ends[0], roll(g1, 1, 1) if i == NB - 1 else S[4, i])
        w0 = (g1z - g1) - (g2y - g2) + f0
        w1 = (g2_lo - g2) - (g0z - g0) + f1
        w2 = (g0y - g0) - (g1_lo - g1) + f2
        return w0, w1, w2

    def divergence(i, f, lo, ends):
        f1y = below_y(f[1], LOW[2, i : i + 1, :])
        f2z = first_lane(ends[2], S[5, i])
        return IDN[i] * ((lo[2] - f[0]) + (f1y - f[1]) + (f2z - f[2]))

    def one_round(j, carry):
        receive(j, (6, 7, 8, 9, 10, 11))
        scale = jnp.where(j == 0, F32(1.0 / SIGMA), F32(2.0 / SIGMA))
        rows_above(j)
        slabs = edges(j, False)

        def products(i):
            ends = halo(slabs, i)
            c, u = fluxes(j, i, ends)
            for n in range(3):
                U[j, n, i] = u[n]
            return [K[n, i] * c[n] for n in range(3)], [M[n, i] * u[n] for n in range(3)], ends

        def advance(i, slab, g, f, ends, lo):
            w = operator(i, g, f, lo, ends)
            q = divergence(i, f, lo, ends)
            w = [scale * w[n] - T[n, i] for n in range(3)]
            for n in range(3):
                V[j + 1, n, i] = w[n]
            s = {n: w[n] * ID[n, i] for n in range(3)}
            s[3] = scale * q - T[3, i]
            if i == 0:
                del s[1], s[2]
            if i == NB - 1:
                del s[0]
            return finish(j + 1, i, slab, s)

        slab = jnp.zeros((ROWS, LANES), F32)
        g, f, ends = products(0)
        plane_0 = (g, f, ends)
        for i in range(1, NB):
            lo = (g[1], g[2], f[0])
            if i == NB - 1:
                receive(j, (4, 5))
            g, f, ends = products(i)
            slab = advance(i, slab, g, f, ends, lo)
        slab = advance(0, slab, *plane_0, fluxes_low(j, False))
        receive(j, (0, 1, 2, 3))
        end = NB - 1
        xz = jnp.where(lane_id() == 0, CZ7[...] * from_lanes(DR[j, 3], 0), 0.0)
        xy = jnp.where(row_id() == 0, CY[1, end : end + 1, :] * DXR[j, 1], 0.0)
        w0 = V[j + 1, 0, end] - scale * (xy + xz)
        xy = jnp.where(row_id() == 31, CX[1, 31:32, :] * DXR[j, 0], 0.0)
        w1 = V[j + 1, 1, 0] - scale * xy
        xz = jnp.where(lane_id() == 127, CX[0] * from_lanes(DR[j, 2], 127), 0.0)
        w2 = V[j + 1, 2, 0] - scale * xz
        s0, s1, s2 = w0 * ID[0, end], w1 * ID[1, 0], w2 * ID[2, 0]
        diagonals(j + 1, s0, s1, s2)
        send(j + 1, (0, 1, 2, 3))
        slab = finish(j + 1, end, slab, {0: s0})
        slab = finish(j + 1, 0, slab, {1: s1, 2: s2})
        send(j + 1, (5, 4))
        V[j + 1, 0, end], V[j + 1, 1, 0], V[j + 1, 2, 0] = w0, w1, w2
        ZS[j + 1] = slab
        send(j + 1, LATE)
        ahead(j + 1)
        wu = jnp.zeros((8, LANES), F32)
        for i in range(NB):
            w = [V[j + 1, n, i] for n in range(3)]
            wu = wu + fold(w[0] * U[j, 0, i] + w[1] * U[j, 1, i] + w[2] * U[j, 2, i])
        MOM[pl.ds(2 * j + 1, 1), :] = jnp.sum(wu, axis=0, keepdims=True)
        return carry

    last = ITERS - 1
    ahead(0)
    lax.fori_loop(0, last, one_round, 0)

    core = lax.rem(gz, 2)
    group_a = [
        (dx, 0, 0 if dc == 0 else 1 - 2 * core)
        for dx in range(nx)
        for dc in range(2)
        if (dx, dc) != (0, 0)
    ]
    pair = [(0, 0, 1 - 2 * core)]
    chips = [
        (dx, dy, dz)
        for dx in range(nx)
        for dy in range(ny)
        for dz in range(0, nz, 2)
        if (dx, dy, dz) != (0, 0, 0)
    ]
    chips.sort(key=lambda o: -sum(min(d, n - d) for d, n in zip((o[0], o[1], o[2] // 2), (nx, ny, nz // 2))))
    group_b = [(0, dy, dz) for dy in range(ny) for dz in range(0, nz, 2) if (dy, dz) != (0, 0)]

    def spread(n, group, base, into):
        copies = [
            remote(SUM.at[n], into.at[k], a_send.at[base + k], a_recv.at[base + k], offset)
            for k, offset in enumerate(group)
        ]
        for c in copies:
            c.start()
        return copies

    def gather(n, copies, into):
        total = SUM[n]
        at = len(copies)
        while at > 0:
            low = max(0, at - 8)
            for k in range(at - 1, low - 1, -1):
                copies[k].wait_recv()
            rows = [into[k] for k in range(low, at)]
            while len(rows) > 1:
                rows = [sum(rows[k + 1 : k + 2], rows[k]) for k in range(0, len(rows), 2)]
            total = total + rows[0]
            at = low
        return total

    n_a, n_b = len(group_a), len(group_b)
    SUM[0] = lanes_of(MOM[...])
    copies_0 = spread(0, group_a, 0, RA)

    receive(last, (9, 11))
    rows_above(last)
    high = ZR[last, 1]
    au = jnp.zeros((8, LANES), F32)
    for i in range(NB):
        if i == NB - 1:
            receive(last, (5,))
        ends = [roll(high, 127 - place(f, i) - 1, 1) for f in (0, 1, 3)]
        c, u = fluxes(last, i, ends)
        g = [K[n, i] * c[n] for n in range(3)]
        f = [M[n, i] * u[n] for n in range(3)]
        for n in range(3):
            U[last, n, i] = u[n]
            G[n, i], G[3 + n, i] = g[n], f[n]
        au = au + fold(
            (g[0] * c[0] + g[1] * c[1] + g[2] * c[2]) + (f[0] * u[0] + f[1] * u[1] + f[2] * u[2])
        )
    au = jnp.sum(jnp.sum(au, axis=0, keepdims=True), axis=1, keepdims=True)
    SUM[1] = jnp.broadcast_to(au, (1, LANES))
    copies_1 = spread(1, pair, n_a + n_b, RC)
    SUM[3] = gather(1, copies_1, RC)
    copies_3 = spread(3, chips, n_a + n_b + 1, RD)
    SUM[2] = gather(0, copies_0, RA)
    copies_2 = spread(2, group_b, n_a, RB)
    receive(last, (0, 1, 2, 3, 6, 7, 8, 10, 4))
    slabs = edges(last, True)
    scale = 2.0 / SIGMA

    def last_planes(planes):
        for i in planes:
            if i == 0:
                lo = fluxes_low(last, True)
            else:
                lo = (G[1, i - 1], G[2, i - 1], G[3, i - 1])
            ends = halo(slabs[0:2], i)
            w = operator(i, [G[n, i] for n in range(3)], [G[3 + n, i] for n in range(3)], lo, ends)
            for n in range(3):
                V[last + 1, n, i] = scale * w[n] - T[n, i]

    last_planes(range(0, NB))
    total = gather(2, copies_2, RB)
    moment = [
        jnp.broadcast_to(jnp.sum(jnp.where(lane_id(1) == m, total, 0.0), axis=1, keepdims=True), (1, LANES))
        for m in range(2 * ITERS - 1)
    ]
    nu = moment[0:2]
    for m in range(2, 2 * ITERS - 1):
        nu.append(2.0 * moment[m] - nu[m % 2])
    cx, cp, cr, ca, gamma, slack, weight = cheb_coefficients(nu)
    for c in range(3):
        for i in range(NB):
            u = [U[j, c, i] for j in range(ITERS)]
            v = [V[j, c, i] for j in range(ITERS + 1)]
            x_out[c, i] = sum(cx[j] * u[j] for j in range(1, last)) + cx[0] * u[0]
            p_out[c, i] = sum(cp[j] * u[j] for j in range(1, ITERS)) + cp[0] * u[0]
            r_out[c, i] = sum(cr[j] * v[j] for j in range(1, ITERS)) + cr[0] * v[0]
            a_out[c, i] = sum(ca[j] * v[j] for j in range(1, ITERS + 1)) + ca[0] * v[0]

    def sent(j, carry):
        for c in messages(j, range(12)):
            c.wait_send()
        return carry

    lax.fori_loop(0, ITERS, sent, 0)
    for c in coef + copies_0 + copies_1 + copies_2:
        c.wait_send()
    au = gather(3, copies_3, RD)
    top = scale * (au - THETA * moment[2 * last]) - moment[2 * last - 1]
    alpha_out[...] = gamma / (slack + weight * (2.0 * top - nu[1]))
    for c in copies_3:
        c.wait_send()


def epilogue(x, p, r, a, alpha, x_out, r_out, X, R, sem):
    step = alpha[...]
    copies = []
    for c in range(3):
        for i in range(NB):
            X[c, i] = x[c, i] + step * p[c, i]
        copies.append(pltpu.make_async_copy(X.at[c], x_out.at[c], sem.at[2 * c]))
        copies[-1].start()
        for i in range(NB):
            R[c, i] = r[c, i] - step * a[c, i]
        copies.append(pltpu.make_async_copy(R.at[c], r_out.at[c], sem.at[2 * c + 1]))
        copies[-1].start()
    for c in copies:
        c.wait()


def body(sizes, right_side, mass_coef, curl_coef):
    shape = right_side.shape
    nx, ny, nz = sizes
    n_a = 2 * nx - 1
    n_b = ny * nz // 2 - 1
    n_c = nx * ny * nz // 2 - 1
    vm = lambda *s: pltpu.VMEM(s, F32)
    dma = lambda *s: pltpu.SemaphoreType.DMA(s)
    x, p, r, a, alpha = pl.pallas_call(
        functools.partial(kernel, sizes),
        out_shape=(pltpu.VMEM(shape, F32),) * 4 + (pltpu.VMEM((1, LANES), F32),),
        in_specs=[pl.BlockSpec(memory_space=pl.ANY)] * 3,
        out_specs=[pl.BlockSpec(memory_space=pltpu.VMEM)] * 5,
        scratch_shapes=[
            vm(5, *shape),
            vm(*shape),
            vm(*shape),
            vm(*shape),
            vm(*shape[1:]),
            vm(4, 4, 10, 48, LANES),
            vm(4, *shape),
            vm(6, *shape[1:]),
            vm(6, *shape[1:]),
            vm(4, *shape[1:]),
            vm(4, ROWS, LANES),
            vm(4, ROWS, LANES),
            vm(4, 8, LANES),
            vm(4, 8, LANES),
            vm(ROWS, LANES),
            vm(ROWS, LANES),
            vm(3, ROWS, LANES),
            vm(ROWS, LANES),
            vm(4, 7, 8, LANES),
            vm(4, 7, 8, LANES),
            vm(4, ROWS, LANES),
            vm(4, 2, ROWS, LANES),
            vm(4, 4, 8, LANES),
            vm(4, 6, 8, LANES),
            vm(4, 2, 1, LANES),
            vm(4, 2, 1, LANES),
            vm(3, 8, LANES),
            vm(*shape[1:]),
            vm(8, LANES),
            vm(4, 1, LANES),
            vm(n_a, 1, LANES),
            vm(n_b, 1, LANES),
            vm(1, 1, LANES),
            vm(n_c, 1, LANES),
            dma(6),
            dma(3),
            dma(3),
            dma(4, 12),
            dma(4, 12),
            dma(n_a + n_b + 1 + n_c),
            dma(n_a + n_b + 1 + n_c),
        ],
        compiler_params=pltpu.CompilerParams(collective_id=0, has_side_effects=True),
    )(right_side, mass_coef, curl_coef)
    return pl.pallas_call(
        epilogue,
        out_shape=(jax.ShapeDtypeStruct(shape, F32),) * 2,
        in_specs=[pl.BlockSpec(memory_space=pltpu.VMEM)] * 5,
        out_specs=[pl.BlockSpec(memory_space=pl.ANY)] * 2,
        scratch_shapes=[vm(*shape), vm(*shape), dma(6)],
        compiler_params=pltpu.CompilerParams(vmem_limit_bytes=2 << 20),
    )(x, p, r, a, alpha)


def solution(mesh):
    sizes = (mesh.shape["gx"], mesh.shape["gy"], mesh.shape["gz"])
    spec = P(None, "gx", "gy", "gz")
    return jax.shard_map(
        functools.partial(body, sizes),
        mesh=mesh,
        in_specs=(spec,) * 3,
        out_specs=(spec,) * 2,
        check_vma=False,
    )
```
